128 devices in a mesh: seq: 4 (over z_lo, core), ctx: 32 (over y, x, z_hi).
Axes of the slice: x: 4, y: 4, z: 4 (z_hi: 2, z_lo: 2; z = z_hi * 2 + z_lo), core: 2. Of those that a mesh axis runs over, the one named last changes fastest.
Arguments:
- hidden: bfloat16 [131072, 7168], P(('seq', 'ctx')), may hold values from -24 to 24
- router_weight: bfloat16 [7168, 256], replicated, may hold values from -0.0625 to 0.0625
- expert_index: int32 [131072, 8], P(('seq', 'ctx')), may hold values from 0 to 255, all different within a row
- lengths: int32 [4], P('seq'), may hold values from 16384 to 32768
Outputs:
- router_grad: float32 [7168, 256], P('ctx')
- balance: float32 [4], P('seq')
The draws below stay inside these ranges and needn't reach their ends.
Inputs may be any that keep to these rules, and one draw needn't show every extreme that they name: A sequence's valid tokens are its first lengths[s] slots, the rest are padding. `expert_index`: each row names 8 different experts.
All inputs are finite; a program needn't handle non-finite values.
Results may differ from the reference program's by a relative error of at most 0.0003.
Values sent between devices are 32-bit elements; how exact they have to be, the bound alone decides.
No kernel may reach another device: no remote copies, remote signals or barrier semaphores. Data moves between devices by JAX's collectives and lax.ppermute only.
A program may use at most 128 MiB of HBM per device.

```python
import jax
import jax.numpy as jnp
from jax import lax

D = 7168
E = 256
TOPK = 8
LEN = 32768
SEQS = 4
TOKENS = 131072


def place_ends(values, rng, least, largest):
    extent = values.shape
    place = [jax.random.randint(jax.random.fold_in(rng, axis), (), 0, extent[axis]) for axis in range(len(extent))]
    values = values.at[tuple(place)].set(least)
    longest = extent.index(max(extent))
    place[longest] = (place[longest] + 1) % extent[longest]
    return values.at[tuple(place)].set(largest)


def strengthened(array, own_key, source, target, blocks, factor):
    def block_of(axis_at):
        return (jnp.arange(array.shape[axis_at]) // (array.shape[axis_at] // blocks)).reshape((-1,) + (1,) * (array.ndim - 1 - axis_at))

    near = jax.random.permutation(own_key, blocks)[block_of(target)]
    second = (block_of(target) + blocks // 2) % blocks
    return jnp.where((block_of(source) == near) | (block_of(source) == second), factor * array, array)


def block_levels(own_key, dims, shards, smallest, largest):
    level = 1.0
    for axis_at, blocks in shards:
        heights = jax.random.uniform(jax.random.fold_in(jax.random.fold_in(own_key, 6), axis_at), (blocks,), jnp.float32, smallest / len(shards), largest / len(shards))
        level = level * jnp.repeat(jnp.exp(heights), dims[axis_at] // blocks).reshape((-1,) + (1,) * (len(dims) - 1 - axis_at))
    return level


def distinct(rng, rows, amount, top, lift):
    ranking = jax.random.permutation(jax.random.fold_in(rng, 1), amount)
    boost = ranking
    for power in range(3):
        boost = boost * boost // amount
    boost = boost * lift // amount
    lots = jax.random.randint(jax.random.fold_in(rng, 2), (rows, amount), 0, 4096) + boost
    sure = jax.random.permutation(jax.random.fold_in(rng, 3), rows)[jnp.arange(amount) % rows]
    lots = jnp.where(jnp.arange(rows)[:, None] == sure[None, :], 1 << 14, lots)
    priority = lots * amount + jnp.arange(amount)
    return lax.top_k(priority.astype(jnp.int32), top)[1].astype(jnp.int32)


def normal_values(key, dims, spread, most, cuts=(), kind=jnp.bfloat16):
    result = jax.random.normal(key, dims, jnp.float32) * spread
    if len(cuts) > 0:
        result = block_levels(key, dims, cuts, -0.22, 0.18) * result
    return jnp.clip(result, min=-most, max=most).astype(kind)


def heavy_noise(key, dims, spread, most, pieces, heavy, kind=jnp.bfloat16):
    array = spread * jax.random.normal(key, dims, jnp.float32)
    if pieces:
        array = array * block_levels(key, dims, pieces, -0.22, 0.18)
    return jnp.clip(strengthened(array, jax.random.fold_in(key, 3), *heavy), -most, most).astype(kind)


def setup_inputs(seed: int = 0) -> dict:
    keys = jax.random.split(jax.random.key(seed), 5)
    return {
        "hidden": heavy_noise(keys[0], (TOKENS, D), 1.0, 24.0, ((0, 128),), (0, 1, 128, 5.5)),
        "router_weight": normal_values(keys[1], (D, E), D ** -0.5, 0.0625),
        "expert_index": distinct(keys[2], TOKENS, E, TOPK, 256),
        "lengths": place_ends(jax.random.randint(keys[3], (SEQS,), LEN // 2, LEN + 1), jax.random.fold_in(keys[3], 1), LEN // 2, LEN).astype(jnp.int32),
    }


loss_scale = 65536.0


def reference(hidden, router_weight, expert_index, lengths):
    hidden_all = hidden.reshape(SEQS, LEN, D)
    index_all = expert_index.reshape(SEQS, LEN, TOPK)

    def one_sequence(packed):
        hidden_seq, index_seq, length_seq = packed
        tokens_live = length_seq.astype(jnp.float32)
        logits = jnp.dot(hidden_seq, router_weight, preferred_element_type=jnp.float32)
        scores = jax.nn.sigmoid(logits)
        row_total = jnp.sum(scores, axis=1, keepdims=True)
        share_of = scores / row_total
        positions = jnp.arange(LEN, dtype=jnp.int32)
        valid_mask = (positions < length_seq.astype(jnp.int32)).astype(jnp.float32)
        expert_ids = jnp.arange(E, dtype=jnp.int32)
        expert_hits = jnp.sum((index_seq[:, :, None] == expert_ids).astype(jnp.float32), axis=1)
        counts = jnp.sum(valid_mask[:, None] * expert_hits, axis=0)
        score_sum = jnp.sum(valid_mask[:, None] * share_of, axis=0)
        fraction = E * counts / (TOPK * tokens_live)
        mean_score = score_sum / tokens_live
        balance = jnp.sum(fraction * mean_score)
        weights = loss_scale * fraction / tokens_live
        weighted = jnp.sum(weights * share_of, axis=1, keepdims=True)
        grad_logits = (weights - weighted) / row_total * scores * (1.0 - scores) * valid_mask[:, None]
        grad_seq = lax.dot_general(hidden_seq.astype(jnp.float32), grad_logits, (((0,), (0,)), ((), ())), precision=lax.Precision.HIGHEST, preferred_element_type=jnp.float32)
        return balance, grad_seq

    balance, grad_stack = lax.map(one_sequence, (hidden_all, index_all, lengths))
    return jnp.sum(grad_stack, axis=0), balance
```

```python
import functools

import jax
import jax.numpy as jnp
from jax import lax
from jax.experimental import pallas as pl
from jax.experimental.pallas import tpu as pltpu
from jax.sharding import Mesh
from jax.sharding import PartitionSpec as P

E = 256
TOPK = 8
HALF = 128
loss_scale = 65536.0

CTX = ("y", "x", "zh")
Z = ("zl", "zh")


VMEM = pl.BlockSpec(memory_space=pltpu.VMEM)
SMEM = pl.BlockSpec(memory_space=pltpu.SMEM)


def swap(array, axis, k):
    if axis == Z:
        pairs = [(l * 2 + h, (l ^ (k & 1)) * 2 + (h ^ (k >> 1))) for l in range(2) for h in range(2)]
    elif axis == "core":
        pairs = [(0, 1), (1, 0)]
    else:
        pairs = [(i, i ^ k) for i in range(4)]
    return lax.ppermute(array, axis, pairs)


def count_kernel(where, index, out):
    rows = index.shape[0]
    hits = jnp.zeros((rows, E), jnp.float32)
    experts = lax.broadcasted_iota(jnp.int32, (rows, E), 1)
    for k in range(TOPK):
        hits = hits + (index[:, k : k + 1] == experts).astype(jnp.float32)
    position = where[0] + lax.broadcasted_iota(jnp.int32, (8, rows), 1)
    valid = (position < where[1]).astype(jnp.bfloat16)
    counts = jnp.dot(valid, hits.astype(jnp.bfloat16), preferred_element_type=jnp.float32)
    out[...] = counts[:1]


def logits_kernel(hidden, weight, out):
    step = pl.program_id(0)
    part = jnp.dot(hidden[...], weight[...], preferred_element_type=jnp.float32)

    @pl.when(step == 0)
    def _():
        out[...] = part

    @pl.when(step > 0)
    def _():
        out[...] += part


def grad_logits_kernel(where, logits, counts, theirs, mine, balance, turned):
    rows = logits.shape[0]
    live = where[1].astype(jnp.float32)
    fraction = E * jnp.sum(counts[...], axis=0) / (TOPK * live)
    weights = loss_scale * fraction / live
    scores = jax.nn.sigmoid(logits[...])
    total = jnp.sum(scores, axis=1, keepdims=True)
    inverse = 1.0 / total
    weighted = jnp.sum(weights * scores, axis=1, keepdims=True) * inverse
    position = where[0] + lax.broadcasted_iota(jnp.int32, (rows, 1), 0)
    valid = position < where[1]
    grad = jnp.where(valid, (weights - weighted) * inverse * scores * (1.0 - scores), 0.0)
    balance[...] = jnp.broadcast_to(
        jnp.sum(jnp.where(valid, weighted, 0.0), axis=0, keepdims=True) / loss_scale, balance.shape
    )
    turned[...] = grad.T
    for out, half in ((theirs, 1 - where[2]), (mine, where[2])):
        value = turned[pl.ds(pl.multiple_of(half * HALF, HALF), HALF), :]
        high = value.astype(jnp.bfloat16)
        out[:HALF, :] = high
        out[HALF:, :] = (value - high.astype(jnp.float32)).astype(jnp.bfloat16)


def product_kernel(grad, hidden, out):
    both = jnp.dot(grad[...], hidden[...], preferred_element_type=jnp.float32)
    out[...] = (both[:HALF] + both[HALF:]).T


def first_kernel(where, mine, theirs, balance, *outs):
    y, x = where[3], where[4]
    for k in range(4):
        a, b = outs[k], outs[4 + k]
        for i in range(4):
            for z in range(2):
                at = (i * 2 + z) * 112
                a[at : at + 112] = mine[y ^ k, i, z, 0] + theirs[y ^ k, i, z, 0]
                b[at : at + 112] = mine[i, x ^ k, z, 1] + theirs[i, x ^ k, z, 1]
        a[896:904] = balance[...]


def second_kernel(place, extra, where, a0, a1, a2, a3, *outs):
    at = where[place]
    for k in range(4):
        rows = pl.ds(pl.multiple_of((at ^ k) * 224, 8), 224)
        outs[k][:224] = a0[rows] + a1[rows] + a2[rows] + a3[rows]
        if extra:
            outs[k][224:232] = a0[896:904] + a1[896:904] + a2[896:904] + a3[896:904]


def third_kernel(where, a0, a1, a2, a3, b0, b1, b2, b3, same, other):
    zh = where[5]
    for out, block in ((same, zh), (other, 1 - zh)):
        rows = pl.ds(pl.multiple_of(block * 112, 8), 112)
        out[:112] = a0[rows] + a1[rows] + a2[rows] + a3[rows]
        out[112:224] = b0[rows] + b1[rows] + b2[rows] + b3[rows]
        out[224:232] = a0[224:232] + a1[224:232] + a2[224:232] + a3[224:232]


def fourth_kernel(same, r1, r2, r3, out, balance):
    out[...] = same[:224] + r1[:224] + r2[:224] + r3[:224]
    balance[...] = same[224:232] + r2[224:232]


def f32(*dims):
    return jax.ShapeDtypeStruct(dims, jnp.float32)


def shards(hidden, router_weight, expert_index, lengths):
    rows, width = hidden.shape
    y, x, zh = (lax.axis_index(a) for a in CTX)
    core = lax.axis_index("core")
    where = jnp.stack([lax.axis_index(CTX) * rows, lengths[0], core, y, x, zh]).astype(jnp.int32)

    counts = pl.pallas_call(
        count_kernel, out_shape=f32(1, E), in_specs=[SMEM, VMEM], out_specs=VMEM, name="count"
    )(where, expert_index)
    counts = lax.all_to_all(
        jnp.broadcast_to(counts[None], (32, 1, E)), CTX, 0, 0, tiled=True
    )

    depth = 512
    logits = pl.pallas_call(
        logits_kernel,
        grid=(width // depth,),
        out_shape=f32(rows, E),
        in_specs=[
            pl.BlockSpec((rows, depth), lambda i: (0, i)),
            pl.BlockSpec((depth, E), lambda i: (i, 0)),
        ],
        out_specs=pl.BlockSpec((rows, E), lambda i: (0, 0)),
        cost_estimate=pl.CostEstimate(
            flops=2 * rows * width * E, bytes_accessed=2 * rows * width, transcendentals=0
        ),
        name="logits",
    )(hidden, router_weight)

    split = jax.ShapeDtypeStruct((E, rows), jnp.bfloat16)
    grad_theirs, grad_mine, balance = pl.pallas_call(
        grad_logits_kernel,
        out_shape=(split, split, f32(8, HALF)),
        in_specs=[SMEM, VMEM, VMEM],
        out_specs=(VMEM, VMEM, VMEM),
        scratch_shapes=[pltpu.VMEM((E, rows), jnp.float32)],
        name="grad_logits",
    )(where, logits, counts)

    step = 512

    def product(grad, name):
        return pl.pallas_call(
            product_kernel,
            grid=(width // step,),
            out_shape=f32(width, HALF),
            in_specs=[
                pl.BlockSpec((E, rows), lambda i: (0, 0)),
                pl.BlockSpec((rows, step), lambda i: (0, i)),
            ],
            out_specs=pl.BlockSpec((step, HALF), lambda i: (i, 0)),
            cost_estimate=pl.CostEstimate(
                flops=2 * rows * width * E, bytes_accessed=2 * rows * width, transcendentals=0
            ),
            name=name,
        )(grad, hidden)

    theirs = swap(product(grad_theirs, "product_theirs"), "core", 1)
    mine = product(grad_mine, "product_mine")
    mine, theirs = (v.reshape(4, 4, 2, 2, 112, HALF) for v in (mine, theirs))
    first = pl.pallas_call(
        first_kernel,
        out_shape=(f32(904, HALF),) * 4 + (f32(896, HALF),) * 4,
        in_specs=[SMEM, VMEM, VMEM, VMEM],
        out_specs=(VMEM,) * 8,
        name="first",
    )(where, mine, theirs, balance)
    a, b = first[:4], first[4:]
    a = [a[0]] + [swap(a[k], "y", k) for k in (1, 2, 3)]
    b = [b[0]] + [swap(b[k], "x", k) for k in (1, 2, 3)]

    def second(parts, place, extra, name):
        n = 232 if extra else 224
        return pl.pallas_call(
            functools.partial(second_kernel, place, extra),
            out_shape=(f32(n, HALF),) * 4,
            in_specs=[SMEM] + [VMEM] * 4,
            out_specs=(VMEM,) * 4,
            name=name,
        )(where, *parts)

    a = second(a, 4, True, "second_a")
    b = second(b, 3, False, "second_b")
    a = [a[0]] + [swap(a[k], "x", k) for k in (1, 2, 3)]
    b = [b[0]] + [swap(b[k], "y", k) for k in (1, 2, 3)]
    same, other = pl.pallas_call(
        third_kernel,
        out_shape=(f32(232, HALF),) * 2,
        in_specs=[SMEM] + [VMEM] * 8,
        out_specs=(VMEM,) * 2,
        name="third",
    )(where, *a, *b)
    arrived = [swap(other if k > 1 else same, Z, k) for k in (1, 2, 3)]
    half, balance = pl.pallas_call(
        fourth_kernel,
        out_shape=(f32(224, HALF), f32(8, HALF)),
        in_specs=[VMEM] * 4,
        out_specs=(VMEM,) * 2,
        name="fourth",
    )(same, *arrived)
    peer = swap(half, "core", 1)
    router_grad = jnp.where(
        core == 0,
        jnp.concatenate([half, peer], axis=1),
        jnp.concatenate([peer, half], axis=1),
    )
    return router_grad, balance[0, :1]


def solution(mesh):
    finer = Mesh(mesh.devices.reshape(2, 2, 4, 4, 2), ("zl", "core", "y", "x", "zh"))
    rows = ("zl", "core", "y", "x", "zh")
    return jax.shard_map(
        shards,
        mesh=finer,
        in_specs=(P(rows, None), P(), P(rows, None), P(("zl", "core"))),
        out_specs=(P(CTX, None), P(("zl", "core"))),
        check_vma=False,
    )
```

```python
import functools

import jax
import jax.numpy as jnp
from jax import lax
from jax.experimental import pallas as pl
from jax.experimental.pallas import tpu as pltpu
from jax.sharding import Mesh
from jax.sharding import PartitionSpec as P

E = 256
TOPK = 8
HALF = 128
loss_scale = 65536.0

CTX = ("y", "x", "zh")
Z = ("zl", "zh")


MIB = 1 << 20
VMEM = pl.BlockSpec(memory_space=pltpu.VMEM)
SMEM = pl.BlockSpec(memory_space=pltpu.SMEM)


def f32(*dims):
    return jax.ShapeDtypeStruct(dims, jnp.float32)


def local(kernel, outs, *args, name, scalars=0, limit=2, **more):
    specs = (VMEM,) * len(outs) if isinstance(outs, tuple) else VMEM
    return pl.pallas_call(
        kernel,
        out_shape=outs,
        in_specs=[SMEM] * scalars + [VMEM] * (len(args) - scalars),
        out_specs=more.pop("out_specs", specs),
        compiler_params=pltpu.CompilerParams(vmem_limit_bytes=limit * MIB),
        name=name,
        **more,
    )(*args)


def swap(array, axis, k):
    if axis == Z:
        pairs = [(l * 2 + h, (l ^ (k & 1)) * 2 + (h ^ (k >> 1))) for l in range(2) for h in range(2)]
    elif axis == "core":
        pairs = [(0, 1), (1, 0)]
    else:
        pairs = [(i, i ^ k) for i in range(4)]
    return lax.ppermute(array, axis, pairs)


def ds(start, size):
    return pl.ds(pl.multiple_of(start, 8), size)


def count_kernel(length, index, out):
    rows = index.shape[1]
    experts = lax.broadcasted_iota(jnp.int32, (E, rows), 0)
    hits = index[0:1, :] == experts
    for k in range(1, TOPK):
        hits = hits | (index[k : k + 1, :] == experts)
    position = lax.axis_index(CTX) * rows + lax.broadcasted_iota(jnp.int32, (8, rows), 1)
    valid = (position < length[0]).astype(jnp.bfloat16)
    counts = lax.dot_general(
        valid,
        hits.astype(jnp.float32).astype(jnp.bfloat16),
        (((1,), (1,)), ((), ())),
        preferred_element_type=jnp.float32,
    )
    out[...] = counts


def logits_kernel(first, last, hidden, weight, *more):
    depth = 512
    out = more[-1]
    if first == 0:
        out[...] = jnp.dot(
            hidden[:, :depth], weight[:depth], preferred_element_type=jnp.float32
        )

    def body(i, _):
        at = pl.multiple_of(i * depth, depth)
        out[...] += jnp.dot(
            hidden[:, pl.ds(at, depth)], weight[pl.ds(at, depth)], preferred_element_type=jnp.float32
        )
        return 0

    lax.fori_loop(max(first, 1), last, body, 0)


def grad_logits_kernel(length, logits, counts, theirs, mine, balance, turned):
    rows = logits.shape[0]
    live = length[0].astype(jnp.float32)
    fraction = E * counts[:1] / (TOPK * live)
    weights = loss_scale * fraction / live
    scores = jax.nn.sigmoid(logits[...])
    total = jnp.sum(scores, axis=1, keepdims=True)
    inverse = 1.0 / total
    weighted = jnp.sum(weights * scores, axis=1, keepdims=True) * inverse
    position = lax.axis_index(CTX) * rows + lax.broadcasted_iota(jnp.int32, (rows, 1), 0)
    valid = position < length[0]
    grad = jnp.where(valid, (weights - weighted) * inverse * scores * (1.0 - scores), 0.0)
    balance[...] = jnp.broadcast_to(
        jnp.sum(jnp.where(valid, weighted, 0.0), axis=0, keepdims=True) / loss_scale, balance.shape
    )
    turned[...] = grad.T
    core = lax.axis_index("core")
    for out, half in ((theirs, 1 - core), (mine, core)):
        value = turned[ds(half * HALF, HALF), :]
        high = value.astype(jnp.bfloat16)
        out[:HALF, :] = high
        out[HALF:, :] = (value - high.astype(jnp.float32)).astype(jnp.bfloat16)


def product_kernel(grad, hidden, out):
    step = 512

    def body(i, _):
        at = pl.multiple_of(i * step, step)
        both = jnp.dot(grad[...], hidden[:, pl.ds(at, step)], preferred_element_type=jnp.float32)
        out[pl.ds(at, step), :] = (both[:HALF] + both[HALF:]).T
        return 0

    lax.fori_loop(0, hidden.shape[1] // step, body, 0)


def block(mine, theirs, part, p, q, z):
    i, j = (p, q) if part == 0 else (q, p)
    return mine[i, j, z, part] + theirs[i, j, z, part]


def places(part):
    y, x = lax.axis_index("y"), lax.axis_index("x")
    return (y, x) if part == 0 else (x, y)


def lead_kernel(mine, theirs, balance, a1, a3, b1, b3):
    for part, (out1, out3) in enumerate(((a1, a3), (b1, b3))):
        me, _ = places(part)
        for q in range(4):
            out = out1 if q < 2 else out3
            for z in range(2):
                at = (q % 2 * 2 + z) * 112
                out[at : at + 112] = block(mine, theirs, part, me ^ 2, q, z)
    a1[448:456] = balance[...]


def rest_kernel(mine, theirs, *outs):
    for part in range(2):
        me, _ = places(part)
        for n, k in enumerate((0, 1, 3)):
            out = outs[part * 3 + n]
            for q in range(4):
                for z in range(2):
                    at = (q * 2 + z) * 112
                    out[at : at + 112] = block(mine, theirs, part, me ^ k, q, z)


def relay_kernel(t1, t3, r1, r3, *more):
    if len(more) == 3:
        balance, o1, o3 = more
        o3[896:904] = balance[...] + r1[448:456]
    else:
        o1, o3 = more
    o1[:448] = t1[:448]
    o1[448:896] = t1[448:896] + r3[:448]
    o3[:448] = t3[:448] + r1[:448]
    o3[448:896] = t3[448:896]


def second_kernel(part, own, r1, r3, *more):
    _, me = places(part)
    if part == 0:
        balance, first, send, keep = more
        send[448:456] = balance[...] + first[448:456] + r3[896:904]
    else:
        send, keep = more
    for n, (out, k) in enumerate(((send, 1), (send, 2), (keep, 0), (keep, 3))):
        at = n % 2 * 224
        rows = ds((me ^ k) * 224, 224)
        out[at : at + 224] = own[rows] + r1[rows] + r3[rows]


def third_kernel(part, sent, keep, r1, *outs):
    send, own = outs
    own[:224] = keep[:224] + r1[:224]
    send[:224] = keep[224:448] + r1[224:448]
    if part == 0:
        send[224:232] = sent[448:456] + r1[448:456]


def join_kernel(a, ra, sent, b, rb, send, keep):
    zh = lax.axis_index("zh")
    for out, z in ((keep, zh), (send, 1 - zh)):
        rows = ds(z * 112, 112)
        out[:112] = a[rows] + ra[rows]
        out[112:224] = b[rows] + rb[rows]
        out[224:232] = sent[224:232] + ra[224:232]


def pair_kernel(keep, r, send):
    send[:224] = keep[:224] + r[:224]
    send[224:232] = r[224:232]


def half_kernel(keep, sent, r, half, balance):
    half[...] = sent[:224] + r[:224]
    balance[0] = jnp.sum(keep[224:225, :1] + r[224:225, :1])


def last_kernel(half, peer, out):
    core = lax.axis_index("core")
    out[:, pl.ds(pl.multiple_of(core * HALF, HALF), HALF)] = half[...]
    out[:, pl.ds(pl.multiple_of((1 - core) * HALF, HALF), HALF)] = peer[...]


def shards(hidden, router_weight, expert_index, lengths):
    rows, width = hidden.shape

    counts = local(
        count_kernel,
        f32(8, E),
        lengths,
        expert_index.T,
        name="count",
        scalars=1,
        limit=4,
        cost_estimate=pl.CostEstimate(
            flops=10**10, bytes_accessed=10**7, transcendentals=0
        ),
    )
    for axis, k in (("y", 1), ("y", 3), ("x", 1), ("x", 3), (Z, 2)):
        counts = counts + swap(counts, axis, k)

    work = pl.CostEstimate(
        flops=2 * rows * width * E, bytes_accessed=2 * rows * width, transcendentals=0
    )
    hidden = pltpu.with_memory_space_constraint(hidden, pltpu.VMEM)
    router_weight = pltpu.with_memory_space_constraint(router_weight, pltpu.VMEM)
    logits = ()
    for n, (low, high) in enumerate(((0, 4), (4, 9), (9, 14))):
        logits = (
            local(
                functools.partial(logits_kernel, low, high),
                f32(rows, E),
                hidden,
                router_weight,
                *logits,
                name=f"logits_{n}",
                cost_estimate=pl.CostEstimate(
                    flops=work.flops // 3, bytes_accessed=work.bytes_accessed // 3, transcendentals=0
                ),
                input_output_aliases={2: 0} if logits else {},
            ),
        )
    (logits,) = logits

    split = jax.ShapeDtypeStruct((E, rows), jnp.bfloat16)
    grad_theirs, grad_mine, balance = local(
        grad_logits_kernel,
        (split, split, f32(8, HALF)),
        lengths,
        logits,
        counts,
        name="grad_logits",
        scalars=1,
        limit=6,
        scratch_shapes=[pltpu.VMEM((E, rows), jnp.float32)],
    )

    def product(grad, name):
        return local(
            product_kernel, f32(width, HALF), grad, hidden, name=name, cost_estimate=work, limit=3
        )

    theirs = swap(product(grad_theirs, "product_theirs"), "core", 1)
    mine = product(grad_mine, "product_mine")
    mine, theirs = (v.reshape(4, 4, 2, 2, 112, HALF) for v in (mine, theirs))

    a1, a3, b1, b3 = local(
        lead_kernel,
        (f32(456, HALF), f32(448, HALF), f32(448, HALF), f32(448, HALF)),
        mine,
        theirs,
        balance,
        name="lead",
    )
    ra1, ra3 = swap(a1, "y", 1), swap(a3, "y", 3)
    rb1, rb3 = swap(b1, "x", 1), swap(b3, "x", 3)
    a0, ta1, ta3, b0, tb1, tb3 = local(
        rest_kernel, (f32(896, HALF),) * 6, mine, theirs, name="rest"
    )
    sa1, sa3 = local(
        relay_kernel, (f32(896, HALF), f32(904, HALF)), ta1, ta3, ra1, ra3, balance, name="relay_a"
    )
    qa1, qa3 = swap(sa1, "y", 1), swap(sa3, "y", 3)
    sb1, sb3 = local(
        relay_kernel, (f32(896, HALF), f32(896, HALF)), tb1, tb3, rb1, rb3, name="relay_b"
    )
    qb1, qb3 = swap(sb1, "x", 1), swap(sb3, "x", 3)

    send_a, keep_a = local(
        functools.partial(second_kernel, 0),
        (f32(456, HALF), f32(448, HALF)),
        a0,
        qa1,
        qa3,
        balance,
        ra1,
        name="second_a",
    )
    ra = swap(send_a, "x", 1)
    send_b, keep_b = local(
        functools.partial(second_kernel, 1),
        (f32(448, HALF), f32(448, HALF)),
        b0,
        qb1,
        qb3,
        name="second_b",
    )
    rb = swap(send_b, "y", 1)
    last_a, own_a = local(
        functools.partial(third_kernel, 0),
        (f32(232, HALF), f32(224, HALF)),
        send_a,
        keep_a,
        ra,
        name="third_a",
    )
    wa = swap(last_a, "x", 3)
    last_b, own_b = local(
        functools.partial(third_kernel, 1),
        (f32(224, HALF), f32(224, HALF)),
        send_b,
        keep_b,
        rb,
        name="third_b",
    )
    wb = swap(last_b, "y", 3)
    send, keep = local(
        join_kernel, (f32(232, HALF),) * 2, own_a, wa, last_a, own_b, wb, name="join"
    )
    arrived = swap(send, Z, 3)
    pair = local(pair_kernel, f32(232, HALF), keep, arrived, name="pair")
    arrived = swap(pair, Z, 1)
    half, balance = local(
        half_kernel,
        (f32(224, HALF), f32(1)),
        keep,
        pair,
        arrived,
        name="half",
        out_specs=(VMEM, SMEM),
    )
    peer = swap(half, "core", 1)
    return local(last_kernel, f32(224, E), half, peer, name="last"), balance


def solution(mesh):
    finer = Mesh(mesh.devices.reshape(2, 2, 4, 4, 2), ("zl", "core", "y", "x", "zh"))
    rows = ("zl", "core", "y", "x", "zh")
    return jax.shard_map(
        shards,
        mesh=finer,
        in_specs=(P(rows, None), P(), P(rows, None), P(("zl", "core"))),
        out_specs=(P(CTX, None), P(("zl", "core"))),
        check_vma=False,
    )
```

```python
import functools

import jax
import jax.numpy as jnp
from jax import lax
from jax.experimental import pallas as pl
from jax.experimental.pallas import tpu as pltpu
from jax.sharding import Mesh
from jax.sharding import PartitionSpec as P

E = 256
TOPK = 8
HALF = 128
loss_scale = 65536.0

CTX = ("y", "x", "zh")
Z = ("zl", "zh")


MIB = 1 << 20
VMEM = pl.BlockSpec(memory_space=pltpu.VMEM)
SMEM = pl.BlockSpec(memory_space=pltpu.SMEM)


def f32(*dims):
    return jax.ShapeDtypeStruct(dims, jnp.float32)


def local(kernel, outs, *args, scalars=0, limit=2, **more):
    specs = (VMEM,) * len(outs) if isinstance(outs, tuple) else VMEM
    return pl.pallas_call(
        kernel,
        out_shape=outs,
        in_specs=[SMEM] * scalars + [VMEM] * (len(args) - scalars),
        out_specs=more.pop("out_specs", specs),
        compiler_params=pltpu.CompilerParams(vmem_limit_bytes=limit * MIB),
        **more,
    )(*args)


def swap(array, axis, k):
    if axis == Z:
        pairs = [(l * 2 + h, (l ^ (k & 1)) * 2 + (h ^ (k >> 1))) for l in range(2) for h in range(2)]
    elif axis == "core":
        pairs = [(0, 1), (1, 0)]
    else:
        pairs = [(i, i ^ k) for i in range(4)]
    return lax.ppermute(array, axis, pairs)


def ds(start, size):
    return pl.ds(pl.multiple_of(start, 8), size)


def count_kernel(length, index, out):
    rows = index.shape[1]
    experts = lax.broadcasted_iota(jnp.int32, (E, rows), 0)
    hits = index[0:1, :] == experts
    for k in range(1, TOPK):
        hits = hits | (index[k : k + 1, :] == experts)
    position = lax.axis_index(CTX) * rows + lax.broadcasted_iota(jnp.int32, (8, rows), 1)
    valid = (position < length[0]).astype(jnp.bfloat16)
    counts = lax.dot_general(
        valid,
        hits.astype(jnp.float32).astype(jnp.bfloat16),
        (((1,), (1,)), ((), ())),
        preferred_element_type=jnp.float32,
    )
    out[...] = jnp.broadcast_to(counts[:1][None], out.shape)


def front_kernel(length, counts, hidden, weight, theirs, mine, balance, kept, held, logits, turned, sems):
    rows, width = hidden.shape
    depth = 512
    parts = width // depth

    def copies(i):
        at = slice(i * depth, (i + 1) * depth)
        return (
            pltpu.make_async_copy(weight.at[at], held.at[at], sems.at[0, i]),
            pltpu.make_async_copy(hidden.at[:, at], kept.at[:, at], sems.at[1, i]),
        )

    for i in range(parts):
        for copy in copies(i):
            copy.start()
    for i in range(parts):
        for copy in copies(i):
            copy.wait()
        at = slice(i * depth, (i + 1) * depth)
        part = jnp.dot(kept[:, at], held[at], preferred_element_type=jnp.float32)
        if i == 0:
            logits[...] = part
        else:
            logits[...] += part

    live = length[0].astype(jnp.float32)
    fraction = E * jnp.sum(counts[...], axis=0) / (TOPK * live)
    weights = loss_scale * fraction / live
    scores = jax.nn.sigmoid(logits[...])
    total = jnp.sum(scores, axis=1, keepdims=True)
    inverse = 1.0 / total
    weighted = jnp.sum(weights * scores, axis=1, keepdims=True) * inverse
    position = lax.axis_index(CTX) * rows + lax.broadcasted_iota(jnp.int32, (rows, 1), 0)
    valid = position < length[0]
    grad = jnp.where(valid, (weights - weighted) * inverse * scores * (1.0 - scores), 0.0)
    balance[...] = jnp.broadcast_to(
        jnp.sum(jnp.where(valid, weighted, 0.0), axis=0, keepdims=True) / loss_scale, balance.shape
    )
    turned[...] = grad.T
    core = lax.axis_index("core")
    for out, half in ((theirs, 1 - core), (mine, core)):
        value = turned[ds(half * HALF, HALF), :]
        high = value.astype(jnp.bfloat16)
        out[:HALF, :] = high
        out[HALF:, :] = (value - high.astype(jnp.float32)).astype(jnp.bfloat16)


def product_kernel(start, grad, hidden, out):
    step = 512
    for at in range(0, out.shape[0], step):
        columns = hidden[:, start + at : start + at + step]
        both = jnp.dot(grad[...], columns, preferred_element_type=jnp.float32)
        out[at : at + step, :] = (both[:HALF] + both[HALF:]).T


def move(mine, theirs, part, upper, k, out, blocks):
    y, x = lax.axis_index("y"), lax.axis_index("x")
    for n, (q, z) in enumerate(blocks):
        if part == 0:
            i, j, half = y ^ k, q, upper ^ (k >> 1)
            other = theirs[half][i & 1, j, z, 0]
        else:
            i, j = q, x ^ k
            other = theirs[i // 2][i % 2, j, z, 1]
        out[n * 112 : n * 112 + 112] = mine[i, j, z, part] + other


BLOCKS = tuple((q, z) for q in range(4) for z in range(2))


def lead_kernel(mine, low, high, balance, a1, a3, b1, b3):
    for upper in range(2):

        @pl.when(lax.axis_index("y") // 2 == upper)
        def _():
            move(mine, (low, high), 0, upper, 2, a1, BLOCKS[:4])
            move(mine, (low, high), 0, upper, 2, a3, BLOCKS[4:])

    move(mine, (low, high), 1, 0, 2, b1, BLOCKS[:4])
    move(mine, (low, high), 1, 0, 2, b3, BLOCKS[4:])
    a1[448:456] = balance[...]


def rest_kernel(mine, low, high, *outs):
    for upper in range(2):

        @pl.when(lax.axis_index("y") // 2 == upper)
        def _():
            for out, k in zip(outs[:3], (0, 1, 3)):
                move(mine, (low, high), 0, upper, k, out, BLOCKS)

    for out, k in zip(outs[3:], (0, 1, 3)):
        move(mine, (low, high), 1, 0, k, out, BLOCKS)


def relay_kernel(t1, t3, r1, r3, *more):
    if len(more) == 3:
        balance, o1, o3 = more
        o3[896:904] = balance[...] + r1[448:456]
    else:
        o1, o3 = more
    o1[:448] = t1[:448]
    o1[448:896] = t1[448:896] + r3[:448]
    o3[:448] = t3[:448] + r1[:448]
    o3[448:896] = t3[448:896]


def second_kernel(part, own, r1, r3, *more):
    me = lax.axis_index("x" if part == 0 else "y")
    if part == 0:
        balance, first, *outs = more
        sum_so_far = balance[...] + first[448:456] + r3[896:904]
    else:
        outs = more
    for k, out in enumerate(outs):
        rows = ds((me ^ k) * 224, 224)
        out[:224] = own[rows] + r1[rows] + r3[rows]
        if part == 0:
            out[224:232] = sum_so_far


def join_kernel(a0, a1, a2, a3, b0, b1, b2, b3, same, other):
    zh = lax.axis_index("zh")
    for out, z in ((same, zh), (other, 1 - zh)):
        rows = ds(z * 112, 112)
        out[:112] = a0[rows] + a1[rows] + a2[rows] + a3[rows]
        out[112:224] = b0[rows] + b1[rows] + b2[rows] + b3[rows]
        out[224:232] = a0[224:232] + a1[224:232] + a2[224:232] + a3[224:232]


def half_kernel(same, r1, r2, r3, half, balance):
    half[...] = same[:224] + r1[:224] + r2[:224] + r3[:224]
    balance[0] = jnp.sum(same[224:225, :1] + r2[224:225, :1])


def last_kernel(half, peer, out):
    core = lax.axis_index("core")
    out[:, pl.ds(pl.multiple_of(core * HALF, HALF), HALF)] = half[...]
    out[:, pl.ds(pl.multiple_of((1 - core) * HALF, HALF), HALF)] = peer[...]


def shards(hidden, router_weight, expert_index, lengths):
    rows, width = hidden.shape

    counts = local(count_kernel, f32(32, 1, E), lengths, expert_index.T, scalars=1, limit=4)
    counts = lax.all_to_all(counts, CTX, 0, 0, tiled=True)

    hidden = pltpu.with_memory_space_constraint(hidden, pltpu.HBM)
    router_weight = pltpu.with_memory_space_constraint(router_weight, pltpu.HBM)
    split = jax.ShapeDtypeStruct((E, rows), jnp.bfloat16)
    away = pl.BlockSpec(memory_space=pltpu.HBM)
    grad_theirs, grad_mine, balance, hidden = pl.pallas_call(
        front_kernel,
        out_shape=(split, split, f32(8, HALF), jax.ShapeDtypeStruct(hidden.shape, hidden.dtype)),
        in_specs=[SMEM, VMEM, away, away],
        out_specs=(VMEM,) * 4,
        scratch_shapes=[
            pltpu.VMEM(router_weight.shape, router_weight.dtype),
            pltpu.VMEM((rows, E), jnp.float32),
            pltpu.VMEM((E, rows), jnp.float32),
            pltpu.SemaphoreType.DMA((2, width // 512)),
        ],
        compiler_params=pltpu.CompilerParams(vmem_limit_bytes=12 * MIB),
        name="front",
    )(lengths, counts, hidden, router_weight)

    def product(grad, start, size):
        work = pl.CostEstimate(flops=size * E, bytes_accessed=size, transcendentals=0)
        return local(
            functools.partial(product_kernel, start),
            f32(size, HALF),
            grad,
            hidden,
            cost_estimate=work,
            limit=3,
        )

    part = width // 2
    low = product(grad_theirs, 0, part)
    low, grad_theirs = lax.optimization_barrier((low, grad_theirs))
    low = swap(low, "core", 1)
    high = product(grad_theirs, part, part)
    high = swap(high, "core", 1)
    mine = product(grad_mine, 0, width)
    mine = mine.reshape(4, 4, 2, 2, 112, HALF)
    low, high = (v.reshape(2, 4, 2, 2, 112, HALF) for v in (low, high))

    a1, a3, b1, b3 = local(
        lead_kernel,
        (f32(456, HALF), f32(448, HALF), f32(448, HALF), f32(448, HALF)),
        mine,
        low,
        high,
        balance,
    )
    ra1, ra3 = swap(a1, "y", 1), swap(a3, "y", 3)
    rb1, rb3 = swap(b1, "x", 1), swap(b3, "x", 3)
    a0, ta1, ta3, b0, tb1, tb3 = local(rest_kernel, (f32(896, HALF),) * 6, mine, low, high)
    sa1, sa3 = local(relay_kernel, (f32(896, HALF), f32(904, HALF)), ta1, ta3, ra1, ra3, balance)
    qa1, qa3 = swap(sa1, "y", 1), swap(sa3, "y", 3)
    sb1, sb3 = local(relay_kernel, (f32(896, HALF), f32(896, HALF)), tb1, tb3, rb1, rb3)
    qb1, qb3 = swap(sb1, "x", 1), swap(sb3, "x", 3)

    a = local(
        functools.partial(second_kernel, 0), (f32(232, HALF),) * 4, a0, qa1, qa3, balance, ra1
    )
    a = [a[0]] + [swap(a[k], "x", k) for k in (1, 2, 3)]
    b = local(functools.partial(second_kernel, 1), (f32(224, HALF),) * 4, b0, qb1, qb3)
    b = [b[0]] + [swap(b[k], "y", k) for k in (1, 2, 3)]
    same, other = local(join_kernel, (f32(232, HALF),) * 2, *a, *b)
    arrived = [swap(other if k > 1 else same, Z, k) for k in (1, 2, 3)]
    half, balance = local(
        half_kernel, (f32(224, HALF), f32(1)), same, *arrived, out_specs=(VMEM, SMEM)
    )
    peer = swap(half, "core", 1)
    return local(last_kernel, f32(224, E), half, peer), balance


def solution(mesh):
    finer = Mesh(mesh.devices.reshape(2, 2, 4, 4, 2), ("zl", "core", "y", "x", "zh"))
    rows = ("zl", "core", "y", "x", "zh")
    return jax.shard_map(
        shards,
        mesh=finer,
        in_specs=(P(rows, None), P(), P(rows, None), P(("zl", "core"))),
        out_specs=(P(CTX, None), P(("zl", "core"))),
        check_vma=False,
    )
```

```python
import functools

import jax
import jax.numpy as jnp
from jax import lax
from jax.experimental import pallas as pl
from jax.experimental.pallas import tpu as pltpu
from jax.sharding import Mesh
from jax.sharding import PartitionSpec as P

E = 256
TOPK = 8
HALF = 128
loss_scale = 65536.0

CTX = ("y", "x", "zh")
Z = ("zl", "zh")


MIB = 1 << 20
VMEM = pl.BlockSpec(memory_space=pltpu.VMEM)
SMEM = pl.BlockSpec(memory_space=pltpu.SMEM)


def f32(*dims):
    return jax.ShapeDtypeStruct(dims, jnp.float32)


def local(kernel, outs, *args, scalars=0, limit=2, **more):
    specs = (VMEM,) * len(outs) if isinstance(outs, tuple) else VMEM
    return pl.pallas_call(
        kernel,
        out_shape=outs,
        in_specs=[SMEM] * scalars + [VMEM] * (len(args) - scalars),
        out_specs=more.pop("out_specs", specs),
        compiler_params=pltpu.CompilerParams(vmem_limit_bytes=limit * MIB),
        **more,
    )(*args)


def swap(array, axis, k):
    if axis == Z:
        pairs = [(l * 2 + h, (l ^ (k & 1)) * 2 + (h ^ (k >> 1))) for l in range(2) for h in range(2)]
    elif axis == "core":
        pairs = [(0, 1), (1, 0)]
    else:
        pairs = [(i, i ^ k) for i in range(4)]
    return lax.ppermute(array, axis, pairs)


def ds(start, size):
    return pl.ds(pl.multiple_of(start, 8), size)


def count_kernel(length, index, out):
    rows = index.shape[1]
    experts = lax.broadcasted_iota(jnp.int32, (E, rows), 0)
    hits = index[0:1, :] == experts
    for k in range(1, TOPK):
        hits = hits | (index[k : k + 1, :] == experts)
    position = lax.axis_index(CTX) * rows + lax.broadcasted_iota(jnp.int32, (8, rows), 1)
    valid = (position < length[0]).astype(jnp.bfloat16)
    counts = lax.dot_general(
        valid,
        hits.astype(jnp.float32).astype(jnp.bfloat16),
        (((1,), (1,)), ((), ())),
        preferred_element_type=jnp.float32,
    )
    out[...] = counts


def logits_kernel(start, stop, hidden, weight, *more):
    part = jnp.dot(
        hidden[:, start:stop], weight[start:stop], preferred_element_type=jnp.float32
    )
    if start == 0:
        more[0][...] = part
    else:
        more[1][...] = more[0][...] + part


def grad_logits_kernel(length, logits, counts, theirs, mine, balance, turned):
    rows = logits.shape[0]
    live = length[0].astype(jnp.float32)
    fraction = E * counts[:1] / (TOPK * live)
    weights = loss_scale * fraction / live
    scores = jax.nn.sigmoid(logits[...])
    total = jnp.sum(scores, axis=1, keepdims=True)
    inverse = 1.0 / total
    weighted = jnp.sum(weights * scores, axis=1, keepdims=True) * inverse
    position = lax.axis_index(CTX) * rows + lax.broadcasted_iota(jnp.int32, (rows, 1), 0)
    valid = position < length[0]
    grad = jnp.where(valid, (weights - weighted) * inverse * scores * (1.0 - scores), 0.0)
    balance[...] = jnp.broadcast_to(
        jnp.sum(jnp.where(valid, weighted, 0.0), axis=0, keepdims=True) / loss_scale, balance.shape
    )
    turned[...] = grad.T
    core = lax.axis_index("core")
    for out, half in ((theirs, 1 - core), (mine, core)):
        value = turned[ds(half * HALF, HALF), :]
        high = value.astype(jnp.bfloat16)
        out[:HALF, :] = high
        out[HALF:, :] = (value - high.astype(jnp.float32)).astype(jnp.bfloat16)


def product_kernel(far, grad, hidden, out):
    step = 512
    upper = lax.axis_index("y") // 2
    base = (1 - upper if far else upper) * out.shape[0]
    for at in range(0, out.shape[0], step):
        columns = hidden[:, pl.ds(pl.multiple_of(base + at, HALF), step)]
        both = jnp.dot(grad[...], columns, preferred_element_type=jnp.float32)
        out[at : at + step, :] = (both[:HALF] + both[HALF:]).T


def move(mine, theirs, part, i, j, z, out, at):
    out[at : at + 112] = mine[i, j, z, part] + theirs[i, j, z, part]


def lead_far_kernel(mine, theirs, balance, a1, a3, b1):
    y, x = lax.axis_index("y"), lax.axis_index("x")
    for n in range(4):
        q, z = n // 2, n % 2
        move(mine, theirs, 0, y & 1, q, z, a1, n * 112)
        move(mine, theirs, 0, y & 1, q + 2, z, a3, n * 112)
        move(mine, theirs, 1, q, x ^ 2, z, b1, n * 112)
    a1[448:456] = balance[...]


def lead_near_kernel(mine, theirs, b3):
    x = lax.axis_index("x")
    for n in range(4):
        move(mine, theirs, 1, n // 2, x ^ 2, n % 2, b3, n * 112)


def rest_kernel(mine_far, mine_near, far, near, *outs):
    y, x = lax.axis_index("y"), lax.axis_index("x")
    for n, k in enumerate((0, 1, 3)):
        mine, theirs = (mine_far, far) if k == 3 else (mine_near, near)
        for m in range(8):
            q, z = m // 2, m % 2
            move(mine, theirs, 0, (y ^ k) & 1, q, z, outs[n], m * 112)
            if q < 2:
                move(mine_far, far, 1, q, x ^ k, z, outs[3 + n], m * 112)
            else:
                move(mine_near, near, 1, q - 2, x ^ k, z, outs[3 + n], m * 112)


def relay_kernel(t1, t3, r1, r3, *more):
    if len(more) == 3:
        balance, o1, o3 = more
        o3[896:904] = balance[...] + r1[448:456]
    else:
        o1, o3 = more
    o1[:448] = t1[:448]
    o1[448:896] = t1[448:896] + r3[:448]
    o3[:448] = t3[:448] + r1[:448]
    o3[448:896] = t3[448:896]


def second_kernel(part, own, r1, r3, *more):
    if part == 0:
        me = lax.axis_index("x")
        balance, first, *outs = more
        sum_so_far = balance[...] + first[448:456] + r3[896:904]
    else:
        me = lax.axis_index("y")
        outs = more
    for k, out in enumerate(outs):
        at = me ^ k if part == 0 else ((me ^ k) & 1) + (0 if k > 1 else 2)
        rows = ds(at * 224, 224)
        out[:224] = own[rows] + r1[rows] + r3[rows]
        if part == 0:
            out[224:232] = sum_so_far


def join_kernel(a0, a1, a2, a3, b0, b1, b2, b3, same, other):
    zh = lax.axis_index("zh")
    for out, z in ((same, zh), (other, 1 - zh)):
        rows = ds(z * 112, 112)
        out[:112] = a0[rows] + a1[rows] + a2[rows] + a3[rows]
        out[112:224] = b0[rows] + b1[rows] + b2[rows] + b3[rows]
        out[224:232] = a0[224:232] + a1[224:232] + a2[224:232] + a3[224:232]


def half_kernel(same, r1, r2, r3, half, balance):
    half[...] = same[:224] + r1[:224] + r2[:224] + r3[:224]
    balance[0] = jnp.sum(same[224:225, :1] + r2[224:225, :1])


def last_kernel(half, peer, out):
    core = lax.axis_index("core")
    out[:, pl.ds(pl.multiple_of(core * HALF, HALF), HALF)] = half[...]
    out[:, pl.ds(pl.multiple_of((1 - core) * HALF, HALF), HALF)] = peer[...]


def shards(hidden, router_weight, expert_index, lengths):
    rows, width = hidden.shape

    counts = local(
        count_kernel,
        f32(8, E),
        lengths,
        expert_index.T,
        scalars=1,
        limit=4,
        cost_estimate=pl.CostEstimate(flops=10**10, bytes_accessed=10**7, transcendentals=0),
    )
    hidden = pltpu.with_memory_space_constraint(hidden, pltpu.VMEM)
    router_weight = pltpu.with_memory_space_constraint(router_weight, pltpu.VMEM)
    logits = ()
    cuts = (0, 2048, 4608, width)
    for n, (axis, steps) in enumerate((("y", (1, 3, 2)), ("x", (1, 3, 2)), (Z, (2,)))):
        arrived = [swap(counts, axis, k) for k in steps]
        size = cuts[n + 1] - cuts[n]
        logits = (
            local(
                functools.partial(logits_kernel, cuts[n], cuts[n + 1]),
                f32(rows, E),
                hidden,
                router_weight,
                *logits,
                cost_estimate=pl.CostEstimate(
                    flops=2 * rows * size * E, bytes_accessed=2 * rows * size, transcendentals=0
                ),
                input_output_aliases={2: 0} if logits else {},
            ),
        )
        counts = functools.reduce(jnp.add, arrived, counts)
    (logits,) = logits

    split = jax.ShapeDtypeStruct((E, rows), jnp.bfloat16)
    grad_theirs, grad_mine, balance = local(
        grad_logits_kernel,
        (split, split, f32(8, HALF)),
        lengths,
        logits,
        counts,
        scalars=1,
        limit=6,
        scratch_shapes=[pltpu.VMEM((E, rows), jnp.float32)],
    )

    part = width // 2

    def product(grad, far):
        work = pl.CostEstimate(flops=part * E, bytes_accessed=part, transcendentals=0)
        return local(
            functools.partial(product_kernel, far),
            f32(part, HALF),
            grad,
            hidden,
            cost_estimate=work,
            limit=3,
        )

    def shaped(value):
        return value.reshape(2, 4, 2, 2, 112, HALF)

    far = product(grad_theirs, True)
    far, grad_theirs = lax.optimization_barrier((far, grad_theirs))
    far = swap(far, "core", 1)
    near = product(grad_theirs, False)
    near, grad_mine = lax.optimization_barrier((near, grad_mine))
    near = swap(near, "core", 1)
    mine_far = shaped(product(grad_mine, True))
    far = shaped(far)
    a1, a3, b1 = local(
        lead_far_kernel, (f32(456, HALF), f32(448, HALF), f32(448, HALF)), mine_far, far, balance
    )
    a1, a3, b1, grad_mine = lax.optimization_barrier((a1, a3, b1, grad_mine))
    ra1, ra3 = swap(a1, "y", 1), swap(a3, "y", 3)
    rb1 = swap(b1, "x", 1)
    mine_near = shaped(product(grad_mine, False))
    near = shaped(near)
    b3 = local(lead_near_kernel, f32(448, HALF), mine_near, near)
    rb3 = swap(b3, "x", 3)
    a0, ta1, ta3, b0, tb1, tb3 = local(
        rest_kernel, (f32(896, HALF),) * 6, mine_far, mine_near, far, near
    )
    sa1, sa3 = local(relay_kernel, (f32(896, HALF), f32(904, HALF)), ta1, ta3, ra1, ra3, balance)
    qa1, qa3 = swap(sa1, "y", 1), swap(sa3, "y", 3)
    sb1, sb3 = local(relay_kernel, (f32(896, HALF), f32(896, HALF)), tb1, tb3, rb1, rb3)
    qb1, qb3 = swap(sb1, "x", 1), swap(sb3, "x", 3)

    a = local(
        functools.partial(second_kernel, 0), (f32(232, HALF),) * 4, a0, qa1, qa3, balance, ra1
    )
    a = [a[0]] + [swap(a[k], "x", k) for k in (1, 2, 3)]
    b = local(functools.partial(second_kernel, 1), (f32(224, HALF),) * 4, b0, qb1, qb3)
    b = [b[0]] + [swap(b[k], "y", k) for k in (1, 2, 3)]
    same, other = local(join_kernel, (f32(232, HALF),) * 2, *a, *b)
    arrived = [swap(other if k > 1 else same, Z, k) for k in (1, 2, 3)]
    half, balance = local(
        half_kernel, (f32(224, HALF), f32(1)), same, *arrived, out_specs=(VMEM, SMEM)
    )
    peer = swap(half, "core", 1)
    return local(last_kernel, f32(224, E), half, peer), balance


def solution(mesh):
    finer = Mesh(mesh.devices.reshape(2, 2, 4, 4, 2), ("zl", "core", "y", "x", "zh"))
    rows = ("zl", "core", "y", "x", "zh")

    return jax.shard_map(
        shards,
        mesh=finer,
        in_specs=(P(rows, None), P(), P(rows, None), P(("zl", "core"))),
        out_specs=(P(CTX, None), P(("zl", "core"))),
        check_vma=False,
    )
```

```python
import functools
import itertools

import jax
import jax.numpy as jnp
from jax import lax
from jax.experimental import pallas as pl
from jax.experimental.pallas import tpu as pltpu
from jax.sharding import Mesh
from jax.sharding import PartitionSpec as P

E = 256
TOPK = 8
HALF = 128
loss_scale = 65536.0

MESH = ("zl", "core", "y", "x", "zh")
CTX = ("y", "x", "zh")
Z = ("zl", "zh")


MIB = 1 << 20
VMEM = pl.BlockSpec(memory_space=pltpu.VMEM)
SMEM = pl.BlockSpec(memory_space=pltpu.SMEM)


def f32(*dims):
    return jax.ShapeDtypeStruct(dims, jnp.float32)


def local(kernel, outs, *args, scalars=0, limit=2, **more):
    specs = (VMEM,) * len(outs) if isinstance(outs, tuple) else VMEM
    return pl.pallas_call(
        kernel,
        out_shape=outs,
        in_specs=[SMEM] * scalars + [VMEM] * (len(args) - scalars),
        out_specs=more.pop("out_specs", specs),
        compiler_params=pltpu.CompilerParams(vmem_limit_bytes=limit * MIB),
        **more,
    )(*args)


def swap(array, axis, k):
    if axis == Z:
        pairs = [(l * 2 + h, (l ^ (k & 1)) * 2 + (h ^ (k >> 1))) for l in range(2) for h in range(2)]
    elif axis == "core":
        pairs = [(0, 1), (1, 0)]
    else:
        pairs = [(i, i ^ k) for i in range(4)]
    return lax.ppermute(array, axis, pairs)


def cross(array, stage, k):
    shape = (2, 2, 4, 4, 2)
    pairs = []
    for place in itertools.product(*map(range, shape)):
        other = list(place)
        other[2 if place[1] == stage else 3] ^= k
        pairs.append(tuple(functools.reduce(lambda n, i: n * shape[i] + p[i], range(5), 0) for p in (place, other)))
    return lax.ppermute(array, MESH, pairs)


def ds(start, size):
    return pl.ds(pl.multiple_of(start, 8), size)


def count_kernel(length, index, out):
    rows = index.shape[1]
    experts = lax.broadcasted_iota(jnp.int32, (E, rows), 0)
    hits = index[0:1, :] == experts
    for k in range(1, TOPK):
        hits = hits | (index[k : k + 1, :] == experts)
    position = lax.axis_index(CTX) * rows + lax.broadcasted_iota(jnp.int32, (8, rows), 1)
    valid = (position < length[0]).astype(jnp.bfloat16)
    counts = lax.dot_general(
        valid,
        hits.astype(jnp.float32).astype(jnp.bfloat16),
        (((1,), (1,)), ((), ())),
        preferred_element_type=jnp.float32,
    )
    out[...] = counts


def logits_kernel(start, stop, hidden, weight, *more):
    part = jnp.dot(
        hidden[:, start:stop], weight[start:stop], preferred_element_type=jnp.float32
    )
    if start == 0:
        more[0][...] = part
    else:
        more[1][...] = more[0][...] + part


def grad_logits_kernel(length, logits, counts, theirs, mine, balance, turned):
    rows = logits.shape[0]
    live = length[0].astype(jnp.float32)
    fraction = E * counts[:1] / (TOPK * live)
    weights = loss_scale * fraction / live
    scores = jax.nn.sigmoid(logits[...])
    total = jnp.sum(scores, axis=1, keepdims=True)
    inverse = 1.0 / total
    weighted = jnp.sum(weights * scores, axis=1, keepdims=True) * inverse
    position = lax.axis_index(CTX) * rows + lax.broadcasted_iota(jnp.int32, (rows, 1), 0)
    valid = position < length[0]
    grad = jnp.where(valid, (weights - weighted) * inverse * scores * (1.0 - scores), 0.0)
    balance[...] = jnp.broadcast_to(
        jnp.sum(jnp.where(valid, weighted, 0.0), axis=0, keepdims=True) / loss_scale, balance.shape
    )
    turned[...] = grad.T
    core = lax.axis_index("core")
    for out, half in ((theirs, 1 - core), (mine, core)):
        value = turned[ds(half * HALF, HALF), :]
        high = value.astype(jnp.bfloat16)
        out[:HALF, :] = high
        out[HALF:, :] = (value - high.astype(jnp.float32)).astype(jnp.bfloat16)


def places():
    y, x, core = lax.axis_index("y"), lax.axis_index("x"), lax.axis_index("core")
    return jnp.where(core == 0, y, x), jnp.where(core == 0, x, y)


def product_kernel(far, own, grad, hidden, out):
    core = lax.axis_index("core")
    over_y = core == (0 if own else 1)
    half = jnp.where(over_y, lax.axis_index("y"), lax.axis_index("x")) // 2
    half = 1 - half if far else half

    def column(tile):
        run = jnp.where(over_y, half * 4 + tile // 7, tile // 7 * 2 + half)
        return pl.ds(pl.multiple_of(run * 896 + tile % 7 * HALF, HALF), HALF)

    for n in range(0, 28, 4):
        columns = jnp.concatenate([hidden[:, column(n + i)] for i in range(4)], axis=1)
        both = jnp.dot(grad[...], columns, preferred_element_type=jnp.float32)
        out[n * HALF : (n + 4) * HALF, :] = (both[:HALF] + both[HALF:]).T


def run_of(p, q, z):
    core = lax.axis_index("core")
    return ds(
        (p & 1) * jnp.where(core == 0, 1792, 448) + q * jnp.where(core == 0, 448, 896) + z * 224,
        224,
    )


QUARTERS = tuple((q, z) for q in range(2) for z in range(2))


def move(out, mine, theirs, p, upper, more=None):
    for n, (q, z) in enumerate(QUARTERS):
        rows = run_of(p, q + 2 * upper, z)
        at = slice(n * 224, n * 224 + 224)
        value = mine[rows] + theirs[rows]
        out[at] = value if more is None else value + more[at]


def lead_far_kernel(mine, theirs, balance, s1, s3, o3):
    p, _ = places()
    move(s1, mine, theirs, p ^ 2, 0)
    s1[896:904] = balance[...]
    move(s3, mine, theirs, p ^ 2, 1)
    move(o3, mine, theirs, p ^ 3, 1)


def lead_near_kernel(mine, theirs, o1):
    p, _ = places()
    move(o1, mine, theirs, p ^ 1, 0)


def relay_kernel(mine_far, far, mine_near, near, balance, r1, r3, m1, m3):
    p, _ = places()
    move(m1, mine_near, near, p ^ 1, 1, r3)
    move(m3, mine_far, far, p ^ 3, 0, r1)
    m3[896:904] = balance[...] + r1[896:904]


def second_kernel(mine, theirs, o1, m3, m1, o3, balance, r1, *outs):
    p, q = places()
    sum_so_far = balance[...] + r1[896:904] + m3[896:904]
    for upper in range(2):

        @pl.when(q // 2 == upper)
        def _():
            for k, out in enumerate(outs):
                arrived = (o1, m3) if upper ^ (k >> 1) == 0 else (m1, o3)
                for z in range(2):
                    mine_rows = run_of(p, q ^ k, z)
                    rows = ds(((q ^ k) & 1) * 448 + z * 224, 224)
                    out[z * 224 : z * 224 + 224] = (
                        mine[mine_rows] + theirs[mine_rows] + arrived[0][rows] + arrived[1][rows]
                    )

    for out in outs:
        out[448:456] = sum_so_far


def join_kernel(a0, a1, a2, a3, same, other):
    zh = lax.axis_index("zh")
    for out, z in ((same, zh), (other, 1 - zh)):
        rows = ds(z * 224, 224)
        out[:224] = a0[rows] + a1[rows] + a2[rows] + a3[rows]
        out[224:232] = a0[448:456] + a1[448:456] + a2[448:456] + a3[448:456]


def half_kernel(same, r1, r2, r3, half, balance):
    half[...] = same[:224] + r1[:224] + r2[:224] + r3[:224]
    balance[0] = jnp.sum(same[224:225, :1] + r2[224:225, :1])


def last_kernel(half, peer, out):
    core = lax.axis_index("core")
    out[:, pl.ds(pl.multiple_of(core * HALF, HALF), HALF)] = half[...]
    out[:, pl.ds(pl.multiple_of((1 - core) * HALF, HALF), HALF)] = peer[...]


def shards(hidden, router_weight, expert_index, lengths):
    rows, width = hidden.shape

    counts = local(
        count_kernel,
        f32(8, E),
        lengths,
        expert_index.T,
        scalars=1,
        limit=4,
        cost_estimate=pl.CostEstimate(flops=10**10, bytes_accessed=10**7, transcendentals=0),
    )
    hidden = pltpu.with_memory_space_constraint(hidden, pltpu.VMEM)
    router_weight = pltpu.with_memory_space_constraint(router_weight, pltpu.VMEM)
    logits = ()
    cuts = (0, 2048, 4608, width)
    for n, (axis, steps) in enumerate((("y", (1, 3, 2)), ("x", (1, 3, 2)), (Z, (2,)))):
        arrived = [swap(counts, axis, k) for k in steps]
        size = cuts[n + 1] - cuts[n]
        logits = (
            local(
                functools.partial(logits_kernel, cuts[n], cuts[n + 1]),
                f32(rows, E),
                hidden,
                router_weight,
                *logits,
                cost_estimate=pl.CostEstimate(
                    flops=2 * rows * size * E, bytes_accessed=2 * rows * size, transcendentals=0
                ),
                input_output_aliases={2: 0} if logits else {},
            ),
        )
        counts = functools.reduce(jnp.add, arrived, counts)
    (logits,) = logits

    split = jax.ShapeDtypeStruct((E, rows), jnp.bfloat16)
    grad_theirs, grad_mine, balance = local(
        grad_logits_kernel,
        (split, split, f32(8, HALF)),
        lengths,
        logits,
        counts,
        scalars=1,
        limit=6,
        scratch_shapes=[pltpu.VMEM((E, rows), jnp.float32)],
    )

    part = width // 2

    def product(grad, far, own):
        work = pl.CostEstimate(flops=part * E, bytes_accessed=part, transcendentals=0)
        return local(
            functools.partial(product_kernel, far, own),
            f32(part, HALF),
            grad,
            hidden,
            cost_estimate=work,
            limit=3,
        )

    far = product(grad_theirs, True, False)
    far, grad_theirs = lax.optimization_barrier((far, grad_theirs))
    far = swap(far, "core", 1)
    near = product(grad_theirs, False, False)
    near, grad_mine = lax.optimization_barrier((near, grad_mine))
    near = swap(near, "core", 1)
    mine_far = product(grad_mine, True, True)
    s1, s3, o3 = local(
        lead_far_kernel, (f32(904, HALF), f32(896, HALF), f32(896, HALF)), mine_far, far, balance
    )
    s1, s3, o3, grad_mine = lax.optimization_barrier((s1, s3, o3, grad_mine))
    r1, r3 = cross(s1, 0, 1), cross(s3, 0, 3)
    o3 = cross(o3, 0, 3)
    mine_near = product(grad_mine, False, True)
    o1 = local(lead_near_kernel, f32(896, HALF), mine_near, near)
    o1 = cross(o1, 0, 1)
    m1, m3 = local(
        relay_kernel,
        (f32(896, HALF), f32(904, HALF)),
        mine_far,
        far,
        mine_near,
        near,
        balance,
        r1,
        r3,
    )
    m1, m3 = cross(m1, 0, 1), cross(m3, 0, 3)
    a = local(second_kernel, (f32(456, HALF),) * 4, mine_near, near, o1, m3, m1, o3, balance, r1)
    a = [a[0]] + [cross(a[k], 1, k) for k in (1, 2, 3)]
    same, other = local(join_kernel, (f32(232, HALF),) * 2, *a)
    arrived = [swap(other if k > 1 else same, Z, k) for k in (1, 2, 3)]
    half, balance = local(
        half_kernel, (f32(224, HALF), f32(1)), same, *arrived, out_specs=(VMEM, SMEM)
    )
    peer = swap(half, "core", 1)
    return local(last_kernel, f32(224, E), half, peer), balance


def solution(mesh):
    finer = Mesh(mesh.devices.reshape(2, 2, 4, 4, 2), MESH)
    rows = MESH

    return jax.shard_map(
        shards,
        mesh=finer,
        in_specs=(P(rows, None), P(), P(rows, None), P(("zl", "core"))),
        out_specs=(P(CTX, None), P(("zl", "core"))),
        check_vma=False,
    )
```

```python
import functools
import itertools

import jax
import jax.numpy as jnp
from jax import lax
from jax.experimental import pallas as pl
from jax.experimental.pallas import tpu as pltpu
from jax.sharding import Mesh
from jax.sharding import PartitionSpec as P

E = 256
TOPK = 8
HALF = 128
loss_scale = 65536.0

MESH = ("zl", "core", "y", "x", "zh")
CTX = ("y", "x", "zh")
Z = ("zl", "zh")


MIB = 1 << 20
VMEM = pl.BlockSpec(memory_space=pltpu.VMEM)
SMEM = pl.BlockSpec(memory_space=pltpu.SMEM)


def f32(*dims):
    return jax.ShapeDtypeStruct(dims, jnp.float32)


def local(kernel, outs, *args, scalars=0, limit=2, **more):
    specs = (VMEM,) * len(outs) if isinstance(outs, tuple) else VMEM
    return pl.pallas_call(
        kernel,
        out_shape=outs,
        in_specs=[SMEM] * scalars + [VMEM] * (len(args) - scalars),
        out_specs=more.pop("out_specs", specs),
        compiler_params=pltpu.CompilerParams(vmem_limit_bytes=limit * MIB),
        **more,
    )(*args)


def swap(array, axis, k):
    if axis == Z:
        pairs = [(l * 2 + h, (l ^ (k & 1)) * 2 + (h ^ (k >> 1))) for l in range(2) for h in range(2)]
    elif axis == "core":
        pairs = [(0, 1), (1, 0)]
    else:
        pairs = [(i, i ^ k) for i in range(4)]
    return lax.ppermute(array, axis, pairs)


SHAPE = (2, 2, 4, 4, 2)


def flat(place):
    return functools.reduce(lambda n, i: n * SHAPE[i] + place[i], range(5), 0)


def moved(place, axis, k):
    return tuple(at ^ k if i == axis else at for i, at in enumerate(place))


def cross(array, stage, k):
    places = itertools.product(*map(range, SHAPE))
    pairs = [(flat(p), flat(moved(p, 2 if p[1] == stage else 3, k))) for p in places]
    return lax.ppermute(array, MESH, pairs)


def north(array, axis, k):
    place, bits = {"y": (2, k), "x": (3, k), "zh": (4, 1)}[axis]
    pairs = []
    for start in itertools.product(*map(range, SHAPE)):
        if start[1] == 1:
            pairs.append((flat(start), flat(moved(start, place, bits))))
    return lax.ppermute(array, MESH, pairs)


def ds(start, size):
    return pl.ds(pl.multiple_of(start, 8), size)


def count_kernel(length, index, out):
    rows = index.shape[1]
    position = lax.axis_index(CTX) * rows + lax.broadcasted_iota(jnp.int32, (1, rows), 1)
    experts = jnp.where(position < length[0], index[...], -1)
    high, low = experts >> 4, experts & 15
    names = lax.broadcasted_iota(jnp.int32, (16, rows), 0)
    counts = jnp.zeros((16, 16), jnp.float32)
    for k in range(TOPK):
        one, two = (
            (part[k : k + 1, :] == names).astype(jnp.float32).astype(jnp.bfloat16)
            for part in (high, low)
        )
        counts = counts + lax.dot_general(
            one, two, (((1,), (1,)), ((), ())), preferred_element_type=jnp.float32
        )
    lane = lax.broadcasted_iota(jnp.int32, (16, E), 1)
    row = lax.broadcasted_iota(jnp.int32, (16, E), 0)
    wide = jnp.dot(
        counts,
        ((lane & 15) == row).astype(jnp.float32),
        precision=lax.Precision.HIGHEST,
        preferred_element_type=jnp.float32,
    )
    total = jnp.sum(jnp.where((lane >> 4) == row, wide, 0.0), axis=0, keepdims=True)
    out[...] = jnp.broadcast_to(total, out.shape)


def logits_kernel(start, stop, hidden, weight, *more):
    part = jnp.dot(
        hidden[:, start:stop], weight[start:stop], preferred_element_type=jnp.float32
    )
    if start == 0:
        more[0][...] = part
    else:
        more[1][...] = more[0][...] + part


def share_kernel(start, stop, length, hidden, weight, logits, share, slope):
    rows = hidden.shape[0]
    part = jnp.dot(
        hidden[:, start:stop], weight[start:stop], preferred_element_type=jnp.float32
    )
    scores = jax.nn.sigmoid(logits[...] + part)
    inverse = 1.0 / jnp.sum(scores, axis=1, keepdims=True)
    position = lax.axis_index(CTX) * rows + lax.broadcasted_iota(jnp.int32, (rows, 1), 0)
    value = jnp.where(position < length[0], scores * inverse, 0.0)
    share[...] = value
    slope[...] = value * (1.0 - scores)


def grad_logits_kernel(length, share, slope, north, south, theirs, mine, balance, turned):
    core = lax.axis_index("core")
    counts = jnp.where(core == 1, north[:1], south[4:5])
    live = length[0].astype(jnp.float32)
    fraction = E * counts / (TOPK * live)
    weights = loss_scale * fraction / live
    weighted = jnp.sum(weights * share[...], axis=1, keepdims=True)
    turned[...] = ((weights - weighted) * slope[...]).T
    balance[...] = jnp.broadcast_to(
        jnp.sum(weighted, axis=0, keepdims=True) / loss_scale, balance.shape
    )
    for out, half in ((theirs, 1 - core), (mine, core)):
        value = turned[ds(half * HALF, HALF), :]
        high = value.astype(jnp.bfloat16)
        out[:HALF, :] = high
        out[HALF:, :] = (value - high.astype(jnp.float32)).astype(jnp.bfloat16)


def places():
    y, x, core = lax.axis_index("y"), lax.axis_index("x"), lax.axis_index("core")
    return jnp.where(core == 0, y, x), jnp.where(core == 0, x, y)


def product_kernel(far, own, grad, hidden, out):
    core = lax.axis_index("core")
    over_y = core == (0 if own else 1)
    half = jnp.where(over_y, lax.axis_index("y"), lax.axis_index("x")) // 2
    half = 1 - half if far else half

    def columns(tile, size):
        run = jnp.where(over_y, half * 4 + tile // 7, tile // 7 * 2 + half)
        return hidden[:, pl.ds(pl.multiple_of(run * 896 + tile % 7 * HALF, HALF), size)]

    def multiply(block):
        both = jnp.dot(grad[...], block, preferred_element_type=jnp.float32)
        return (both[:HALF] + both[HALF:]).T

    for tile in (0, 14):
        for at in (tile, tile + 2, tile + 4, tile + 7, tile + 9, tile + 11):
            out[at * HALF : (at + 2) * HALF, :] = multiply(columns(at, 2 * HALF))
        ends = jnp.concatenate([columns(tile + n, HALF) for n in (6, 13)], axis=1)
        ends = multiply(ends)
        for n, at in enumerate((tile + 6, tile + 13)):
            out[at * HALF : (at + 1) * HALF, :] = ends[n * HALF : (n + 1) * HALF]


def run_of(p, q, z):
    core = lax.axis_index("core")
    return ds(
        (p & 1) * jnp.where(core == 0, 1792, 448) + q * jnp.where(core == 0, 448, 896) + z * 224,
        224,
    )


QUARTERS = tuple((q, z) for q in range(2) for z in range(2))


def move(out, mine, theirs, p, upper, more=None):
    for n, (q, z) in enumerate(QUARTERS):
        rows = run_of(p, q + 2 * upper, z)
        at = slice(n * 224, n * 224 + 224)
        value = mine[rows] + theirs[rows]
        out[at] = value if more is None else value + more[at]


def lead_far_kernel(mine, theirs, balance, s1, s3, o3):
    p, _ = places()
    move(s1, mine, theirs, p ^ 2, 0)
    s1[896:904] = balance[...]
    move(s3, mine, theirs, p ^ 2, 1)
    move(o3, mine, theirs, p ^ 3, 1)


def lead_near_kernel(mine, theirs, o1):
    p, _ = places()
    move(o1, mine, theirs, p ^ 1, 0)


def relay_kernel(mine_far, far, mine_near, near, balance, r1, r3, m1, m3):
    p, _ = places()
    move(m1, mine_near, near, p ^ 1, 1, r3)
    move(m3, mine_far, far, p ^ 3, 0, r1)
    m3[896:904] = balance[...] + r1[896:904]


def second_kernel(mine, theirs, o1, m3, m1, o3, balance, r1, *outs):
    p, q = places()
    sum_so_far = balance[...] + r1[896:904] + m3[896:904]
    for upper in range(2):

        @pl.when(q // 2 == upper)
        def _():
            for k, out in enumerate(outs):
                arrived = (o1, m3) if upper ^ (k >> 1) == 0 else (m1, o3)
                for z in range(2):
                    mine_rows = run_of(p, q ^ k, z)
                    rows = ds(((q ^ k) & 1) * 448 + z * 224, 224)
                    out[z * 224 : z * 224 + 224] = (
                        mine[mine_rows] + theirs[mine_rows] + arrived[0][rows] + arrived[1][rows]
                    )

    for out in outs:
        out[448:456] = sum_so_far


def join_kernel(a0, a1, a2, a3, same, other):
    zh = lax.axis_index("zh")
    for out, z in ((same, zh), (other, 1 - zh)):
        rows = ds(z * 224, 224)
        out[:224] = a0[rows] + a1[rows] + a2[rows] + a3[rows]
        out[224:232] = a0[448:456] + a1[448:456] + a2[448:456] + a3[448:456]


def half_kernel(same, r1, r2, r3, half):
    half[...] = same[:224] + r1[:224] + r2[:224] + r3[:224]


def balance_kernel(same, r2, balance):
    balance[0] = jnp.sum(same[224:225, :1] + r2[224:225, :1])


def last_kernel(half, peer, out):
    core = lax.axis_index("core")
    out[:, pl.ds(pl.multiple_of(core * HALF, HALF), HALF)] = half[...]
    out[:, pl.ds(pl.multiple_of((1 - core) * HALF, HALF), HALF)] = peer[...]


def shards(hidden, router_weight, expert_index, lengths):
    rows, width = hidden.shape

    counts = local(
        count_kernel,
        f32(8, E),
        lengths,
        expert_index.T,
        scalars=1,
        limit=4,
        cost_estimate=pl.CostEstimate(flops=10**10, bytes_accessed=10**7, transcendentals=0),
    )
    hidden = pltpu.with_memory_space_constraint(hidden, pltpu.VMEM)
    router_weight = pltpu.with_memory_space_constraint(router_weight, pltpu.VMEM)
    mixed = swap(counts, "core", 1)
    own_rows = lax.broadcasted_iota(jnp.int32, counts.shape, 0) < 4
    counts = jnp.where(own_rows, counts, mixed)
    cuts = (0, 1536, 3072, 4608, width)
    parts = ()
    for n, (axis, k) in enumerate((("y", 1), ("y", 3), ("x", 1), ("x", 3), ("zh", 1))):
        arrived = north(counts, axis, k)
        if n > 0:
            low, high = cuts[n - 1 : n + 1]
            final = high == width
            parts = local(
                functools.partial(share_kernel if final else logits_kernel, low, high),
                (f32(rows, E),) * (2 if final else 1),
                *((lengths,) if final else ()),
                hidden,
                router_weight,
                *parts,
                scalars=1 if final else 0,
                limit=4,
                cost_estimate=pl.CostEstimate(
                    flops=2 * rows * (high - low) * E,
                    bytes_accessed=2 * rows * (high - low),
                    transcendentals=0,
                ),
                input_output_aliases={2 + final: 0} if parts else {},
            )
        counts = counts + arrived
    share, slope = parts
    south = lax.ppermute(counts, "core", [(1, 0)])

    split = jax.ShapeDtypeStruct((E, rows), jnp.bfloat16)
    grad_theirs, grad_mine, balance = local(
        grad_logits_kernel,
        (split, split, f32(8, HALF)),
        lengths,
        share,
        slope,
        counts,
        south,
        scalars=1,
        limit=6,
        scratch_shapes=[pltpu.VMEM((E, rows), jnp.float32)],
    )

    part = width // 2

    def product(grad, far, own):
        work = pl.CostEstimate(flops=part * E, bytes_accessed=part, transcendentals=0)
        return local(
            functools.partial(product_kernel, far, own),
            f32(part, HALF),
            grad,
            hidden,
            cost_estimate=work,
            limit=3,
        )

    far = product(grad_theirs, True, False)
    far, grad_theirs = lax.optimization_barrier((far, grad_theirs))
    far = swap(far, "core", 1)
    near = product(grad_theirs, False, False)
    near, grad_mine = lax.optimization_barrier((near, grad_mine))
    near = swap(near, "core", 1)
    mine_far = product(grad_mine, True, True)
    s1, s3, o3 = local(
        lead_far_kernel, (f32(904, HALF), f32(896, HALF), f32(896, HALF)), mine_far, far, balance
    )
    s1, s3, o3, grad_mine = lax.optimization_barrier((s1, s3, o3, grad_mine))
    r1, r3 = cross(s1, 0, 1), cross(s3, 0, 3)
    o3 = cross(o3, 0, 3)
    mine_near = product(grad_mine, False, True)
    o1 = local(lead_near_kernel, f32(896, HALF), mine_near, near)
    o1 = cross(o1, 0, 1)
    m1, m3 = local(
        relay_kernel,
        (f32(896, HALF), f32(904, HALF)),
        mine_far,
        far,
        mine_near,
        near,
        balance,
        r1,
        r3,
    )
    m1, m3 = cross(m1, 0, 1), cross(m3, 0, 3)
    a = local(second_kernel, (f32(456, HALF),) * 4, mine_near, near, o1, m3, m1, o3, balance, r1)
    arrived = {}
    for k in (2, 1, 3):
        arrived[k] = cross(a[k], 1, k)
    same, other = local(
        join_kernel, (f32(232, HALF),) * 2, a[0], arrived[1], arrived[2], arrived[3]
    )
    for k in (2, 1, 3):
        arrived[k] = swap(other if k > 1 else same, Z, k)
    half = local(half_kernel, f32(224, HALF), same, arrived[1], arrived[2], arrived[3])
    peer = swap(half, "core", 1)
    balance = local(balance_kernel, f32(1), same, arrived[2], out_specs=SMEM)
    return local(last_kernel, f32(224, E), half, peer), balance


def solution(mesh):
    finer = Mesh(mesh.devices.reshape(2, 2, 4, 4, 2), MESH)
    rows = MESH

    return jax.shard_map(
        shards,
        mesh=finer,
        in_specs=(P(rows, None), P(), P(rows, None), P(("zl", "core"))),
        out_specs=(P(CTX, None), P(("zl", "core"))),
        check_vma=False,
    )
```

```python
import functools
import itertools

import jax
import jax.numpy as jnp
from jax import lax
from jax.experimental import pallas as pl
from jax.experimental.pallas import tpu as pltpu
from jax.sharding import Mesh
from jax.sharding import PartitionSpec as P

E = 256
TOPK = 8
HALF = 128
loss_scale = 65536.0

MESH = ("zl", "core", "y", "x", "zh")
CTX = ("y", "x", "zh")
Z = ("zl", "zh")


MIB = 1 << 20
VMEM = pl.BlockSpec(memory_space=pltpu.VMEM)
SMEM = pl.BlockSpec(memory_space=pltpu.SMEM)


def f32(*dims):
    return jax.ShapeDtypeStruct(dims, jnp.float32)


def local(kernel, outs, *args, scalars=0, limit=2, **more):
    specs = (VMEM,) * len(outs) if isinstance(outs, tuple) else VMEM
    return pl.pallas_call(
        kernel,
        out_shape=outs,
        in_specs=[SMEM] * scalars + [VMEM] * (len(args) - scalars),
        out_specs=more.pop("out_specs", specs),
        compiler_params=pltpu.CompilerParams(vmem_limit_bytes=limit * MIB),
        **more,
    )(*args)


def swap(array, axis, k):
    if axis == Z:
        pairs = [(l * 2 + h, (l ^ (k & 1)) * 2 + (h ^ (k >> 1))) for l in range(2) for h in range(2)]
    elif axis == "core":
        pairs = [(0, 1), (1, 0)]
    else:
        pairs = [(i, i ^ k) for i in range(4)]
    return lax.ppermute(array, axis, pairs)


SHAPE = (2, 2, 4, 4, 2)


def flat(place):
    return functools.reduce(lambda n, i: n * SHAPE[i] + place[i], range(5), 0)


def moved(place, axis, k):
    return tuple(at ^ k if i == axis else at for i, at in enumerate(place))


def cross(array, stage, k):
    places = itertools.product(*map(range, SHAPE))
    pairs = [(flat(p), flat(moved(p, 2 if p[1] == stage else 3, k))) for p in places]
    return lax.ppermute(array, MESH, pairs)


def north(array, axis, k):
    place, bits = {"y": (2, k), "x": (3, k), "zh": (4, 1)}[axis]
    pairs = []
    for start in itertools.product(*map(range, SHAPE)):
        pairs.append((flat(start), flat(moved(start, place, bits) if start[1] == 1 else start)))
    return lax.ppermute(array, MESH, pairs)


def ds(start, size):
    return pl.ds(pl.multiple_of(start, 8), size)


def count_kernel(length, index, out):
    rows = index.shape[1]
    position = lax.axis_index(CTX) * rows + lax.broadcasted_iota(jnp.int32, (1, rows), 1)
    experts = jnp.where(position < length[0], index[...], -1)
    high, low = experts >> 4, experts & 15
    names = lax.broadcasted_iota(jnp.int32, (16, rows), 0)
    counts = jnp.zeros((16, 16), jnp.float32)
    for k in range(TOPK):
        one, two = (
            (part[k : k + 1, :] == names).astype(jnp.float32).astype(jnp.bfloat16)
            for part in (high, low)
        )
        counts = counts + lax.dot_general(
            one, two, (((1,), (1,)), ((), ())), preferred_element_type=jnp.float32
        )
    lane = lax.broadcasted_iota(jnp.int32, (16, E), 1)
    row = lax.broadcasted_iota(jnp.int32, (16, E), 0)
    wide = jnp.dot(
        counts,
        ((lane & 15) == row).astype(jnp.float32),
        precision=lax.Precision.HIGHEST,
        preferred_element_type=jnp.float32,
    )
    total = jnp.sum(jnp.where((lane >> 4) == row, wide, 0.0), axis=0, keepdims=True)
    out[...] = jnp.broadcast_to(total, out.shape)


def logits_kernel(start, stop, hidden, weight, *more):
    part = jnp.dot(
        hidden[:, start:stop], weight[start:stop], preferred_element_type=jnp.float32
    )
    if start == 0:
        more[0][...] = part
    else:
        more[1][...] = more[0][...] + part


def share_kernel(start, stop, length, hidden, weight, logits, share, slope):
    rows = hidden.shape[0]
    part = jnp.dot(
        hidden[:, start:stop], weight[start:stop], preferred_element_type=jnp.float32
    )
    scores = jax.nn.sigmoid(logits[...] + part)
    inverse = 1.0 / jnp.sum(scores, axis=1, keepdims=True)
    position = lax.axis_index(CTX) * rows + lax.broadcasted_iota(jnp.int32, (rows, 1), 0)
    value = jnp.where(position < length[0], scores * inverse, 0.0)
    share[...] = value
    slope[...] = value * (1.0 - scores)


def grad_logits_kernel(length, share, slope, north, south, theirs, mine, balance, turned):
    core = lax.axis_index("core")
    counts = jnp.where(core == 1, north[:1], south[4:5])
    live = length[0].astype(jnp.float32)
    fraction = E * counts / (TOPK * live)
    weights = loss_scale * fraction / live
    weighted = jnp.sum(weights * share[...], axis=1, keepdims=True)
    turned[...] = ((weights - weighted) * slope[...]).T
    balance[...] = jnp.broadcast_to(
        jnp.sum(weighted, axis=0, keepdims=True) / loss_scale, balance.shape
    )
    for out, half in ((theirs, 1 - core), (mine, core)):
        value = turned[ds(half * HALF, HALF), :]
        high = value.astype(jnp.bfloat16)
        out[:HALF, :] = high
        out[HALF:, :] = (value - high.astype(jnp.float32)).astype(jnp.bfloat16)


def places():
    y, x, core = lax.axis_index("y"), lax.axis_index("x"), lax.axis_index("core")
    return jnp.where(core == 0, y, x), jnp.where(core == 0, x, y)


def product_kernel(k, own, grad, hidden, out, whole):
    over_y = lax.axis_index("core") == (0 if own else 1)
    p = jnp.where(over_y, lax.axis_index("y"), lax.axis_index("x")) ^ k
    for q in range(4):
        start = jnp.where(over_y, p * 1792 + q * 448, q * 1792 + p * 448)
        skip = start & 64
        columns = hidden[:, pl.ds(pl.multiple_of(start - skip, HALF), 512)]
        both = jnp.dot(grad[...], columns, preferred_element_type=jnp.float32)
        whole[q] = (both[:HALF] + both[HALF:]).T
        out[q * 448 : q * 448 + 448, :] = whole[q, ds(skip, 448), :]


LOW, HIGH = slice(0, 896), slice(896, 1792)


def lead_kernel(mine, theirs, balance, s1, s3):
    s1[:896] = mine[LOW] + theirs[LOW]
    s1[896:904] = balance[...]
    s3[...] = mine[HIGH] + theirs[HIGH]


def direct_kernel(rows, mine, theirs, out):
    out[...] = mine[rows] + theirs[rows]


def relay_kernel(mine1, theirs1, mine3, theirs3, balance, r1, r3, m1, m3):
    m1[...] = mine1[HIGH] + theirs1[HIGH] + r3[...]
    m3[:896] = mine3[LOW] + theirs3[LOW] + r1[:896]
    m3[896:904] = balance[...] + r1[896:904]


def second_kernel(mine, theirs, o1, m3, m1, o3, balance, r1, *outs):
    _, q = places()
    sum_so_far = balance[...] + r1[896:904] + m3[896:904]
    for upper in range(2):

        @pl.when(q // 2 == upper)
        def _():
            for k, out in enumerate(outs):
                arrived = (o1, m3) if upper ^ (k >> 1) == 0 else (m1, o3)
                own = ds((q ^ k) * 448, 448)
                rows = ds(((q ^ k) & 1) * 448, 448)
                out[:448] = mine[own] + theirs[own] + arrived[0][rows] + arrived[1][rows]

    for out in outs:
        out[448:456] = sum_so_far


def join_kernel(a0, a1, a2, a3, same, other):
    zh = lax.axis_index("zh")
    for out, z in ((same, zh), (other, 1 - zh)):
        rows = ds(z * 224, 224)
        out[:224] = a0[rows] + a1[rows] + a2[rows] + a3[rows]
        out[224:232] = a0[448:456] + a1[448:456] + a2[448:456] + a3[448:456]


def half_kernel(same, r1, r2, r3, half):
    half[...] = same[:224] + r1[:224] + r2[:224] + r3[:224]


def balance_kernel(same, r2, balance):
    balance[0] = jnp.sum(same[224:225, :1] + r2[224:225, :1])


def last_kernel(half, peer, out):
    core = lax.axis_index("core")
    out[:, pl.ds(pl.multiple_of(core * HALF, HALF), HALF)] = half[...]
    out[:, pl.ds(pl.multiple_of((1 - core) * HALF, HALF), HALF)] = peer[...]


def shards(hidden, router_weight, expert_index, lengths):
    rows, width = hidden.shape

    counts = local(
        count_kernel,
        f32(8, E),
        lengths,
        expert_index.T,
        scalars=1,
        limit=4,
        cost_estimate=pl.CostEstimate(flops=10**10, bytes_accessed=10**7, transcendentals=0),
    )
    hidden = pltpu.with_memory_space_constraint(hidden, pltpu.VMEM)
    router_weight = pltpu.with_memory_space_constraint(router_weight, pltpu.VMEM)
    mixed = swap(counts, "core", 1)
    own_rows = lax.broadcasted_iota(jnp.int32, counts.shape, 0) < 4
    counts = jnp.where(own_rows, counts, mixed)
    cuts = (0, 1536, 3072, 4608, width)
    parts = ()
    for n, (axis, k) in enumerate((("y", 1), ("y", 3), ("x", 1), ("x", 3), ("zh", 1))):
        arrived = north(counts, axis, k)
        if n > 0:
            low, high = cuts[n - 1 : n + 1]
            final = high == width
            parts = local(
                functools.partial(share_kernel if final else logits_kernel, low, high),
                (f32(rows, E),) * (2 if final else 1),
                *((lengths,) if final else ()),
                hidden,
                router_weight,
                *parts,
                scalars=1 if final else 0,
                limit=4,
                cost_estimate=pl.CostEstimate(
                    flops=2 * rows * (high - low) * E,
                    bytes_accessed=2 * rows * (high - low),
                    transcendentals=0,
                ),
                input_output_aliases={2 + final: 0} if parts else {},
            )
        counts = counts + arrived
    share, slope = parts
    south = swap(counts, "core", 1)

    split = jax.ShapeDtypeStruct((E, rows), jnp.bfloat16)
    grad_theirs, grad_mine, balance = local(
        grad_logits_kernel,
        (split, split, f32(8, HALF)),
        lengths,
        share,
        slope,
        counts,
        south,
        scalars=1,
        limit=6,
        scratch_shapes=[pltpu.VMEM((E, rows), jnp.float32)],
    )

    def product(grad, k, own):
        work = pl.CostEstimate(flops=width * E, bytes_accessed=width, transcendentals=0)
        return local(
            functools.partial(product_kernel, k, own),
            f32(width // 4, HALF),
            grad,
            hidden,
            cost_estimate=work,
            limit=4,
            scratch_shapes=[pltpu.VMEM((4, 512, HALF), jnp.float32)],
        )

    mine, theirs = [None] * 4, [None] * 4

    def make_theirs(k):
        made = product(grad_theirs, k, False)
        theirs[k] = swap(made, "core", 1)

    def make_mine(k):
        mine[k] = product(grad_mine, k, True)

    make_theirs(2)
    make_theirs(1)
    make_mine(2)
    s1, s3 = local(lead_kernel, (f32(904, HALF), f32(896, HALF)), mine[2], theirs[2], balance)
    r1, r3 = cross(s1, 0, 1), cross(s3, 0, 3)
    make_theirs(3)
    make_mine(1)
    o1 = local(functools.partial(direct_kernel, LOW), f32(896, HALF), mine[1], theirs[1])
    o1 = cross(o1, 0, 1)
    make_mine(3)
    o3 = local(functools.partial(direct_kernel, HIGH), f32(896, HALF), mine[3], theirs[3])
    o3 = cross(o3, 0, 3)
    make_theirs(0)
    m1, m3 = local(
        relay_kernel,
        (f32(896, HALF), f32(904, HALF)),
        mine[1],
        theirs[1],
        mine[3],
        theirs[3],
        balance,
        r1,
        r3,
    )
    m1, m3 = cross(m1, 0, 1), cross(m3, 0, 3)
    make_mine(0)
    a = local(second_kernel, (f32(456, HALF),) * 4, mine[0], theirs[0], o1, m3, m1, o3, balance, r1)
    arrived = {}
    for k in (2, 1, 3):
        arrived[k] = cross(a[k], 1, k)
    same, other = local(
        join_kernel, (f32(232, HALF),) * 2, a[0], arrived[1], arrived[2], arrived[3]
    )
    for k in (2, 1, 3):
        arrived[k] = swap(other if k > 1 else same, Z, k)
    half = local(half_kernel, f32(224, HALF), same, arrived[1], arrived[2], arrived[3])
    peer = swap(half, "core", 1)
    balance = local(balance_kernel, f32(1), same, arrived[2], out_specs=SMEM)
    return local(last_kernel, f32(224, E), half, peer), balance


def solution(mesh):
    finer = Mesh(mesh.devices.reshape(2, 2, 4, 4, 2), MESH)
    rows = MESH

    return jax.shard_map(
        shards,
        mesh=finer,
        in_specs=(P(rows, None), P(), P(rows, None), P(("zl", "core"))),
        out_specs=(P(CTX, None), P(("zl", "core"))),
        check_vma=False,
    )
```

```python
import functools
import itertools

import jax
import jax.numpy as jnp
from jax import lax
from jax.experimental import pallas as pl
from jax.experimental.pallas import tpu as pltpu
from jax.sharding import Mesh
from jax.sharding import PartitionSpec as P

E = 256
TOPK = 8
HALF = 128
loss_scale = 65536.0

MESH = ("zl", "core", "y", "x", "zh")
CTX = ("y", "x", "zh")
Z = ("zl", "zh")


MIB = 1 << 20
VMEM = pl.BlockSpec(memory_space=pltpu.VMEM)
SMEM = pl.BlockSpec(memory_space=pltpu.SMEM)


def f32(*dims):
    return jax.ShapeDtypeStruct(dims, jnp.float32)


def local(kernel, outs, *args, scalars=0, limit=2, **more):
    specs = (VMEM,) * len(outs) if isinstance(outs, tuple) else VMEM
    return pl.pallas_call(
        kernel,
        out_shape=outs,
        in_specs=[SMEM] * scalars + [VMEM] * (len(args) - scalars),
        out_specs=more.pop("out_specs", specs),
        compiler_params=pltpu.CompilerParams(vmem_limit_bytes=limit * MIB),
        **more,
    )(*args)


def swap(array, axis, k):
    if axis == Z:
        pairs = [(l * 2 + h, (l ^ (k & 1)) * 2 + (h ^ (k >> 1))) for l in range(2) for h in range(2)]
    elif axis == "core":
        pairs = [(0, 1), (1, 0)]
    else:
        pairs = [(i, i ^ k) for i in range(4)]
    return lax.ppermute(array, axis, pairs)


SHAPE = (2, 2, 4, 4, 2)


def flat(place):
    return functools.reduce(lambda n, i: n * SHAPE[i] + place[i], range(5), 0)


def moved(place, axis, k):
    return tuple(at ^ k if i == axis else at for i, at in enumerate(place))


def cross(array, stage, k):
    places = itertools.product(*map(range, SHAPE))
    pairs = [(flat(p), flat(moved(p, 2 if p[1] == stage else 3, k))) for p in places]
    return lax.ppermute(array, MESH, pairs)


def ds(start, size):
    return pl.ds(pl.multiple_of(start, 8), size)


def count_kernel(length, index, out):
    rows = index.shape[1]
    position = lax.axis_index(CTX) * rows + lax.broadcasted_iota(jnp.int32, (1, rows), 1)
    experts = jnp.where(position < length[0], index[...], -1)
    high, low = experts >> 4, experts & 15
    names = lax.broadcasted_iota(jnp.int32, (16, rows), 0)
    counts = jnp.zeros((16, 16), jnp.float32)
    for k in range(TOPK):
        one, two = (
            (part[k : k + 1, :] == names).astype(jnp.float32).astype(jnp.bfloat16)
            for part in (high, low)
        )
        counts = counts + lax.dot_general(
            one, two, (((1,), (1,)), ((), ())), preferred_element_type=jnp.float32
        )
    lane = lax.broadcasted_iota(jnp.int32, (16, E), 1)
    row = lax.broadcasted_iota(jnp.int32, (16, E), 0)
    wide = jnp.dot(
        counts,
        ((lane & 15) == row).astype(jnp.float32),
        precision=lax.Precision.HIGHEST,
        preferred_element_type=jnp.float32,
    )
    total = jnp.sum(jnp.where((lane >> 4) == row, wide, 0.0), axis=0, keepdims=True)
    out[...] = jnp.broadcast_to(total, out.shape)


def logits_kernel(start, stop, hidden, weight, *more):
    part = jnp.dot(
        hidden[:, start:stop], weight[start:stop], preferred_element_type=jnp.float32
    )
    if start == 0:
        more[0][...] = part
    else:
        more[1][...] = more[0][...] + part


def share_kernel(start, stop, length, hidden, weight, logits, share, slope):
    rows = hidden.shape[0]
    part = jnp.dot(
        hidden[:, start:stop], weight[start:stop], preferred_element_type=jnp.float32
    )
    scores = jax.nn.sigmoid(logits[...] + part)
    inverse = 1.0 / jnp.sum(scores, axis=1, keepdims=True)
    position = lax.axis_index(CTX) * rows + lax.broadcasted_iota(jnp.int32, (rows, 1), 0)
    value = jnp.where(position < length[0], scores * inverse, 0.0)
    share[...] = value
    slope[...] = value * (1.0 - scores)


def grad_logits_kernel(length, share, slope, counts, theirs, mine, balance, turned):
    core = lax.axis_index("core")
    live = length[0].astype(jnp.float32)
    fraction = E * counts[:1] / (TOPK * live)
    weights = loss_scale * fraction / live
    weighted = jnp.sum(weights * share[...], axis=1, keepdims=True)
    turned[...] = ((weights - weighted) * slope[...]).T
    balance[...] = jnp.broadcast_to(
        jnp.sum(weighted, axis=0, keepdims=True) / loss_scale, balance.shape
    )
    for out, half in ((theirs, 1 - core), (mine, core)):
        value = turned[ds(half * HALF, HALF), :]
        high = value.astype(jnp.bfloat16)
        out[:HALF, :] = high
        out[HALF:, :] = (value - high.astype(jnp.float32)).astype(jnp.bfloat16)


def places():
    y, x, core = lax.axis_index("y"), lax.axis_index("x"), lax.axis_index("core")
    return jnp.where(core == 0, y, x), jnp.where(core == 0, x, y)


def product_kernel(k, own, grad, hidden, out, whole):
    over_y = lax.axis_index("core") == (0 if own else 1)
    p = jnp.where(over_y, lax.axis_index("y"), lax.axis_index("x")) ^ k
    for q in range(4):
        start = jnp.where(over_y, p * 1792 + q * 448, q * 1792 + p * 448)
        skip = start & 64
        columns = hidden[:, pl.ds(pl.multiple_of(start - skip, HALF), 512)]
        both = jnp.dot(grad[...], columns, preferred_element_type=jnp.float32)
        whole[q] = (both[:HALF] + both[HALF:]).T
        out[q * 448 : q * 448 + 448, :] = whole[q, ds(skip, 448), :]


LOW, HIGH = slice(0, 896), slice(896, 1792)


def lead_kernel(mine, theirs, balance, s1, s3):
    s1[:896] = mine[LOW] + theirs[LOW]
    s1[896:904] = balance[...]
    s3[...] = mine[HIGH] + theirs[HIGH]


def direct_kernel(rows, mine, theirs, out):
    out[...] = mine[rows] + theirs[rows]


def relay_kernel(mine1, theirs1, mine3, theirs3, balance, r1, r3, m1, m3):
    m1[...] = mine1[HIGH] + theirs1[HIGH] + r3[...]
    m3[:896] = mine3[LOW] + theirs3[LOW] + r1[:896]
    m3[896:904] = balance[...] + r1[896:904]


def second_kernel(mine, theirs, o1, m3, m1, o3, balance, r1, *outs):
    _, q = places()
    sum_so_far = balance[...] + r1[896:904] + m3[896:904]
    for upper in range(2):

        @pl.when(q // 2 == upper)
        def _():
            for k, out in enumerate(outs):
                arrived = (o1, m3) if upper ^ (k >> 1) == 0 else (m1, o3)
                own = ds((q ^ k) * 448, 448)
                rows = ds(((q ^ k) & 1) * 448, 448)
                out[:448] = mine[own] + theirs[own] + arrived[0][rows] + arrived[1][rows]

    for out in outs:
        out[448:456] = sum_so_far


def join_kernel(a0, a1, a2, a3, same, other):
    zh = lax.axis_index("zh")
    for out, z in ((same, zh), (other, 1 - zh)):
        rows = ds(z * 224, 224)
        out[:224] = a0[rows] + a1[rows] + a2[rows] + a3[rows]
        out[224:232] = a0[448:456] + a1[448:456] + a2[448:456] + a3[448:456]


def half_kernel(same, r1, r2, r3, half):
    half[...] = same[:224] + r1[:224] + r2[:224] + r3[:224]


def balance_kernel(same, r2, balance):
    balance[0] = jnp.sum(same[224:225, :1] + r2[224:225, :1])


def last_kernel(half, peer, out):
    core = lax.axis_index("core")
    out[:, pl.ds(pl.multiple_of(core * HALF, HALF), HALF)] = half[...]
    out[:, pl.ds(pl.multiple_of((1 - core) * HALF, HALF), HALF)] = peer[...]


def shards(hidden, router_weight, expert_index, lengths):
    rows, width = hidden.shape

    counts = local(
        count_kernel,
        f32(8, E),
        lengths,
        expert_index.T,
        scalars=1,
        limit=4,
        cost_estimate=pl.CostEstimate(flops=10**10, bytes_accessed=10**7, transcendentals=0),
    )
    hidden = pltpu.with_memory_space_constraint(hidden, pltpu.VMEM)
    router_weight = pltpu.with_memory_space_constraint(router_weight, pltpu.VMEM)
    cuts = (0, 2048, 4608, width)
    parts = ()
    for n, (axis, steps) in enumerate((("y", (2, 1, 3)), ("x", (2, 1, 3)), (Z, (2,)))):
        arrived = [swap(counts, axis, k) for k in steps]
        low, high = cuts[n : n + 2]
        final = high == width
        parts = local(
            functools.partial(share_kernel if final else logits_kernel, low, high),
            (f32(rows, E),) * (2 if final else 1),
            *((lengths,) if final else ()),
            hidden,
            router_weight,
            *parts,
            scalars=1 if final else 0,
            limit=4,
            cost_estimate=pl.CostEstimate(
                flops=2 * rows * (high - low) * E,
                bytes_accessed=2 * rows * (high - low),
                transcendentals=0,
            ),
            input_output_aliases={2 + final: 0} if parts else {},
        )
        counts = functools.reduce(jnp.add, arrived, counts)
    share, slope = parts

    split = jax.ShapeDtypeStruct((E, rows), jnp.bfloat16)
    grad_theirs, grad_mine, balance = local(
        grad_logits_kernel,
        (split, split, f32(8, HALF)),
        lengths,
        share,
        slope,
        counts,
        scalars=1,
        limit=6,
        scratch_shapes=[pltpu.VMEM((E, rows), jnp.float32)],
    )

    def product(grad, k, own):
        work = pl.CostEstimate(flops=width * E, bytes_accessed=width, transcendentals=0)
        return local(
            functools.partial(product_kernel, k, own),
            f32(width // 4, HALF),
            grad,
            hidden,
            cost_estimate=work,
            limit=4,
            scratch_shapes=[pltpu.VMEM((4, 512, HALF), jnp.float32)],
        )

    mine, theirs = [None] * 4, [None] * 4

    def make_theirs(k):
        made = product(grad_theirs, k, False)
        theirs[k] = swap(made, "core", 1)

    def make_mine(k):
        mine[k] = product(grad_mine, k, True)

    make_theirs(2)
    make_theirs(1)
    make_mine(2)
    s1, s3 = local(lead_kernel, (f32(904, HALF), f32(896, HALF)), mine[2], theirs[2], balance)
    r1, r3 = cross(s1, 0, 1), cross(s3, 0, 3)
    make_theirs(3)
    make_mine(1)
    o1 = local(functools.partial(direct_kernel, LOW), f32(896, HALF), mine[1], theirs[1])
    o1 = cross(o1, 0, 1)
    make_mine(3)
    o3 = local(functools.partial(direct_kernel, HIGH), f32(896, HALF), mine[3], theirs[3])
    o3 = cross(o3, 0, 3)
    m1, m3 = local(
        relay_kernel,
        (f32(896, HALF), f32(904, HALF)),
        mine[1],
        theirs[1],
        mine[3],
        theirs[3],
        balance,
        r1,
        r3,
    )
    m1, m3 = cross(m1, 0, 1), cross(m3, 0, 3)
    make_theirs(0)
    make_mine(0)
    a = local(second_kernel, (f32(456, HALF),) * 4, mine[0], theirs[0], o1, m3, m1, o3, balance, r1)
    arrived = {}
    for k in (2, 1, 3):
        arrived[k] = cross(a[k], 1, k)
    same, other = local(
        join_kernel, (f32(232, HALF),) * 2, a[0], arrived[1], arrived[2], arrived[3]
    )
    for k in (2, 1, 3):
        arrived[k] = swap(other if k > 1 else same, Z, k)
    half = local(half_kernel, f32(224, HALF), same, arrived[1], arrived[2], arrived[3])
    peer = swap(half, "core", 1)
    balance = local(balance_kernel, f32(1), same, arrived[2], out_specs=SMEM)
    return local(last_kernel, f32(224, E), half, peer), balance


def solution(mesh):
    finer = Mesh(mesh.devices.reshape(2, 2, 4, 4, 2), MESH)
    rows = MESH

    return jax.shard_map(
        shards,
        mesh=finer,
        in_specs=(P(rows, None), P(), P(rows, None), P(("zl", "core"))),
        out_specs=(P(CTX, None), P(("zl", "core"))),
        check_vma=False,
    )
```

```python
import functools
import itertools

import jax
import jax.numpy as jnp
from jax import lax
from jax.experimental import pallas as pl
from jax.experimental.pallas import tpu as pltpu
from jax.sharding import Mesh
from jax.sharding import PartitionSpec as P

E = 256
TOPK = 8
HALF = 128
loss_scale = 65536.0

MESH = ("zl", "core", "y", "x", "zh")
CTX = ("y", "x", "zh")
Z = ("zl", "zh")


MIB = 1 << 20
VMEM = pl.BlockSpec(memory_space=pltpu.VMEM)
SMEM = pl.BlockSpec(memory_space=pltpu.SMEM)


def f32(*dims):
    return jax.ShapeDtypeStruct(dims, jnp.float32)


def local(kernel, outs, *args, scalars=0, limit=2, **more):
    specs = (VMEM,) * len(outs) if isinstance(outs, tuple) else VMEM
    return pl.pallas_call(
        kernel,
        out_shape=outs,
        in_specs=[SMEM] * scalars + [VMEM] * (len(args) - scalars),
        out_specs=more.pop("out_specs", specs),
        compiler_params=pltpu.CompilerParams(vmem_limit_bytes=limit * MIB),
        **more,
    )(*args)


def swap(array, axis, k):
    if axis == Z:
        pairs = [(l * 2 + h, (l ^ (k & 1)) * 2 + (h ^ (k >> 1))) for l in range(2) for h in range(2)]
    elif axis == "core":
        pairs = [(0, 1), (1, 0)]
    else:
        pairs = [(i, i ^ k) for i in range(4)]
    return lax.ppermute(array, axis, pairs)


SHAPE = (2, 2, 4, 4, 2)


def flat(place):
    return functools.reduce(lambda n, i: n * SHAPE[i] + place[i], range(5), 0)


def moved(place, axis, k):
    return tuple(at ^ k if i == axis else at for i, at in enumerate(place))


def cross(array, stage, k):
    places = itertools.product(*map(range, SHAPE))
    pairs = [(flat(p), flat(moved(p, 2 if p[1] == stage else 3, k))) for p in places]
    return lax.ppermute(array, MESH, pairs)


def ds(start, size):
    return pl.ds(pl.multiple_of(start, 8), size)


def count_kernel(length, index, out):
    rows = index.shape[1]
    position = lax.axis_index(CTX) * rows + lax.broadcasted_iota(jnp.int32, (1, rows), 1)
    experts = jnp.where(position < length[0], index[...], -1)
    high, low = experts >> 4, experts & 15
    names = lax.broadcasted_iota(jnp.int32, (16, rows), 0)
    counts = jnp.zeros((16, 16), jnp.float32)
    for k in range(TOPK):
        one, two = (
            (part[k : k + 1, :] == names).astype(jnp.float32).astype(jnp.bfloat16)
            for part in (high, low)
        )
        counts = counts + lax.dot_general(
            one, two, (((1,), (1,)), ((), ())), preferred_element_type=jnp.float32
        )
    lane = lax.broadcasted_iota(jnp.int32, (16, E), 1)
    row = lax.broadcasted_iota(jnp.int32, (16, E), 0)
    wide = jnp.dot(
        counts,
        ((lane & 15) == row).astype(jnp.float32),
        precision=lax.Precision.HIGHEST,
        preferred_element_type=jnp.float32,
    )
    total = jnp.sum(jnp.where((lane >> 4) == row, wide, 0.0), axis=0, keepdims=True)
    out[...] = jnp.broadcast_to(total, out.shape)


def logits_kernel(start, stop, hidden, weight, *more):
    part = jnp.dot(
        hidden[:, start:stop], weight[start:stop], preferred_element_type=jnp.float32
    )
    if start == 0:
        more[0][...] = part
    else:
        more[1][...] = more[0][...] + part


def share_kernel(start, stop, length, hidden, weight, logits, share, slope):
    rows = hidden.shape[0]
    part = jnp.dot(
        hidden[:, start:stop], weight[start:stop], preferred_element_type=jnp.float32
    )
    scores = jax.nn.sigmoid(logits[...] + part)
    inverse = 1.0 / jnp.sum(scores, axis=1, keepdims=True)
    position = lax.axis_index(CTX) * rows + lax.broadcasted_iota(jnp.int32, (rows, 1), 0)
    value = jnp.where(position < length[0], scores * inverse, 0.0)
    share[...] = value
    slope[...] = value * (1.0 - scores)


def grad_logits_kernel(length, share, slope, counts, theirs, mine, balance, turned):
    core = lax.axis_index("core")
    live = length[0].astype(jnp.float32)
    fraction = E * counts[:1] / (TOPK * live)
    weights = loss_scale * fraction / live
    weighted = jnp.sum(weights * share[...], axis=1, keepdims=True)
    turned[...] = ((weights - weighted) * slope[...]).T
    balance[...] = jnp.broadcast_to(
        jnp.sum(weighted, axis=0, keepdims=True) / loss_scale, balance.shape
    )
    for out, half in ((theirs, 1 - core), (mine, core)):
        value = turned[ds(half * HALF, HALF), :]
        high = value.astype(jnp.bfloat16)
        out[:HALF, :] = high
        out[HALF:, :] = (value - high.astype(jnp.float32)).astype(jnp.bfloat16)


def places():
    y, x, core = lax.axis_index("y"), lax.axis_index("x"), lax.axis_index("core")
    return jnp.where(core == 0, y, x), jnp.where(core == 0, x, y)


PAD = 64


def product_kernel(k, own, grad, hidden, out):
    over_y = lax.axis_index("core") == (0 if own else 1)
    p = jnp.where(over_y, lax.axis_index("y"), lax.axis_index("x")) ^ k
    backward = jnp.where(over_y, 0, p & 1) == 1
    for n in range(4):
        q = jnp.where(backward, 3 - n, n)
        start = jnp.where(over_y, p * 1792 + q * 448, q * 1792 + p * 448)
        skip = start & 64
        columns = hidden[:, pl.ds(pl.multiple_of(start - skip, HALF), 512)]
        both = jnp.dot(grad[...], columns, preferred_element_type=jnp.float32)
        out[ds(PAD + q * 448 - skip, 512), :] = (both[:HALF] + both[HALF:]).T


LOW, HIGH = slice(PAD, PAD + 896), slice(PAD + 896, PAD + 1792)


def lead_kernel(mine, theirs, balance, s1, s3):
    s1[:896] = mine[LOW] + theirs[LOW]
    s1[896:904] = balance[...]
    s3[...] = mine[HIGH] + theirs[HIGH]


def direct_kernel(rows, mine, theirs, out):
    out[...] = mine[rows] + theirs[rows]


def relay_kernel(mine1, theirs1, mine3, theirs3, balance, r1, r3, m1, m3):
    m1[...] = mine1[HIGH] + theirs1[HIGH] + r3[...]
    m3[:896] = mine3[LOW] + theirs3[LOW] + r1[:896]
    m3[896:904] = balance[...] + r1[896:904]


def second_kernel(mine, theirs, o1, m3, m1, o3, balance, r1, *outs):
    _, q = places()
    sum_so_far = balance[...] + r1[896:904] + m3[896:904]
    for upper in range(2):

        @pl.when(q // 2 == upper)
        def _():
            for k, out in enumerate(outs):
                arrived = (o1, m3) if upper ^ (k >> 1) == 0 else (m1, o3)
                own = ds(PAD + (q ^ k) * 448, 448)
                rows = ds(((q ^ k) & 1) * 448, 448)
                out[:448] = mine[own] + theirs[own] + arrived[0][rows] + arrived[1][rows]

    for out in outs:
        out[448:456] = sum_so_far


def join_kernel(a0, a1, a2, a3, same, other):
    zh = lax.axis_index("zh")
    for out, z in ((same, zh), (other, 1 - zh)):
        rows = ds(z * 224, 224)
        out[:224] = a0[rows] + a1[rows] + a2[rows] + a3[rows]
        out[224:232] = a0[448:456] + a1[448:456] + a2[448:456] + a3[448:456]


def half_kernel(same, r1, r2, r3, half):
    half[...] = same[:224] + r1[:224] + r2[:224] + r3[:224]


def balance_kernel(same, r2, balance):
    balance[0] = jnp.sum(same[224:225, :1] + r2[224:225, :1])


def last_kernel(half, peer, out):
    core = lax.axis_index("core")
    out[:, pl.ds(pl.multiple_of(core * HALF, HALF), HALF)] = half[...]
    out[:, pl.ds(pl.multiple_of((1 - core) * HALF, HALF), HALF)] = peer[...]


def shards(hidden, router_weight, expert_index, lengths):
    rows, width = hidden.shape

    counts = local(
        count_kernel,
        f32(8, E),
        lengths,
        expert_index.T,
        scalars=1,
        limit=4,
        cost_estimate=pl.CostEstimate(flops=10**10, bytes_accessed=10**7, transcendentals=0),
    )
    hidden = pltpu.with_memory_space_constraint(hidden, pltpu.VMEM)
    router_weight = pltpu.with_memory_space_constraint(router_weight, pltpu.VMEM)
    cuts = (0, 0, width // 2, width)
    parts = ()
    for n, (axis, steps) in enumerate((("y", (2, 1, 3)), ("x", (2, 1, 3)), (Z, (2,)))):
        arrived = [swap(counts, axis, k) for k in steps]
        low, high = cuts[n : n + 2]
        if high > low:
            final = high == width
            parts = local(
                functools.partial(share_kernel if final else logits_kernel, low, high),
                (f32(rows, E),) * (2 if final else 1),
                *((lengths,) if final else ()),
                hidden,
                router_weight,
                *parts,
                scalars=1 if final else 0,
                limit=4,
                cost_estimate=pl.CostEstimate(
                    flops=2 * rows * (high - low) * E,
                    bytes_accessed=2 * rows * (high - low),
                    transcendentals=0,
                ),
                input_output_aliases={2 + final: 0} if parts else {},
            )
        counts = functools.reduce(jnp.add, arrived, counts)
    share, slope = parts

    split = jax.ShapeDtypeStruct((E, rows), jnp.bfloat16)
    grad_theirs, grad_mine, balance = local(
        grad_logits_kernel,
        (split, split, f32(8, HALF)),
        lengths,
        share,
        slope,
        counts,
        scalars=1,
        limit=6,
        scratch_shapes=[pltpu.VMEM((E, rows), jnp.float32)],
    )

    def product(grad, k, own):
        work = pl.CostEstimate(flops=width * E, bytes_accessed=width, transcendentals=0)
        return local(
            functools.partial(product_kernel, k, own),
            f32(width // 4 + 2 * PAD, HALF),
            grad,
            hidden,
            cost_estimate=work,
            limit=3,
        )

    mine, theirs = [None] * 4, [None] * 4

    def make_theirs(k):
        made = product(grad_theirs, k, False)
        theirs[k] = swap(made, "core", 1)

    def make_mine(k):
        mine[k] = product(grad_mine, k, True)

    make_theirs(2)
    make_theirs(1)
    make_theirs(3)
    make_mine(2)
    s1, s3 = local(lead_kernel, (f32(904, HALF), f32(896, HALF)), mine[2], theirs[2], balance)
    r1, r3 = cross(s1, 0, 1), cross(s3, 0, 3)
    make_mine(1)
    o1 = local(functools.partial(direct_kernel, LOW), f32(896, HALF), mine[1], theirs[1])
    o1 = cross(o1, 0, 1)
    make_mine(3)
    o3 = local(functools.partial(direct_kernel, HIGH), f32(896, HALF), mine[3], theirs[3])
    o3 = cross(o3, 0, 3)
    m1, m3 = local(
        relay_kernel,
        (f32(896, HALF), f32(904, HALF)),
        mine[1],
        theirs[1],
        mine[3],
        theirs[3],
        balance,
        r1,
        r3,
    )
    m1, m3 = cross(m1, 0, 1), cross(m3, 0, 3)
    make_theirs(0)
    make_mine(0)
    a = local(second_kernel, (f32(456, HALF),) * 4, mine[0], theirs[0], o1, m3, m1, o3, balance, r1)
    arrived = {}
    for k in (2, 1, 3):
        arrived[k] = cross(a[k], 1, k)
    same, other = local(
        join_kernel, (f32(232, HALF),) * 2, a[0], arrived[1], arrived[2], arrived[3]
    )
    for k in (2, 1, 3):
        arrived[k] = swap(other if k > 1 else same, Z, k)
    half = local(half_kernel, f32(224, HALF), same, arrived[1], arrived[2], arrived[3])
    peer = swap(half, "core", 1)
    balance = local(balance_kernel, f32(1), same, arrived[2], out_specs=SMEM)
    return local(last_kernel, f32(224, E), half, peer), balance


def solution(mesh):
    finer = Mesh(mesh.devices.reshape(2, 2, 4, 4, 2), MESH)
    rows = MESH

    return jax.shard_map(
        shards,
        mesh=finer,
        in_specs=(P(rows, None), P(), P(rows, None), P(("zl", "core"))),
        out_specs=(P(CTX, None), P(("zl", "core"))),
        check_vma=False,
    )
```

```python
import functools
import itertools

import jax
import jax.numpy as jnp
from jax import lax
from jax.experimental import pallas as pl
from jax.experimental.pallas import tpu as pltpu
from jax.sharding import Mesh
from jax.sharding import PartitionSpec as P

E = 256
TOPK = 8
HALF = 128
loss_scale = 65536.0

MESH = ("zl", "core", "y", "x", "zh")
CTX = ("y", "x", "zh")
Z = ("zl", "zh")


MIB = 1 << 20
VMEM = pl.BlockSpec(memory_space=pltpu.VMEM)
SMEM = pl.BlockSpec(memory_space=pltpu.SMEM)


def f32(*dims):
    return jax.ShapeDtypeStruct(dims, jnp.float32)


def local(kernel, outs, *args, scalars=0, limit=2, **more):
    specs = (VMEM,) * len(outs) if isinstance(outs, tuple) else VMEM
    return pl.pallas_call(
        kernel,
        out_shape=outs,
        in_specs=[SMEM] * scalars + [VMEM] * (len(args) - scalars),
        out_specs=more.pop("out_specs", specs),
        compiler_params=pltpu.CompilerParams(vmem_limit_bytes=limit * MIB),
        **more,
    )(*args)


def swap(array, axis, k):
    if axis == Z:
        pairs = [(l * 2 + h, (l ^ (k & 1)) * 2 + (h ^ (k >> 1))) for l in range(2) for h in range(2)]
    elif axis == "core":
        pairs = [(0, 1), (1, 0)]
    else:
        pairs = [(i, i ^ k) for i in range(4)]
    return lax.ppermute(array, axis, pairs)


SHAPE = (2, 2, 4, 4, 2)


def flat(place):
    return functools.reduce(lambda n, i: n * SHAPE[i] + place[i], range(5), 0)


def moved(place, axis, k):
    return tuple(at ^ k if i == axis else at for i, at in enumerate(place))


def cross(array, stage, k):
    places = itertools.product(*map(range, SHAPE))
    pairs = [(flat(p), flat(moved(p, 2 if p[1] == stage else 3, k))) for p in places]
    return lax.ppermute(array, MESH, pairs)


def ds(start, size):
    return pl.ds(pl.multiple_of(start, 8), size)


def count_kernel(length, index, out):
    rows = index.shape[1]
    position = lax.axis_index(CTX) * rows + lax.broadcasted_iota(jnp.int32, (1, rows), 1)
    experts = jnp.where(position < length[0], index[...], -1)
    high, low = experts >> 4, experts & 15
    names = lax.broadcasted_iota(jnp.int32, (16, rows), 0)
    counts = jnp.zeros((16, 16), jnp.float32)
    for k in range(TOPK):
        one, two = (
            (part[k : k + 1, :] == names).astype(jnp.float32).astype(jnp.bfloat16)
            for part in (high, low)
        )
        counts = counts + lax.dot_general(
            one, two, (((1,), (1,)), ((), ())), preferred_element_type=jnp.float32
        )
    lane = lax.broadcasted_iota(jnp.int32, (16, E), 1)
    row = lax.broadcasted_iota(jnp.int32, (16, E), 0)
    wide = jnp.dot(
        counts,
        ((lane & 15) == row).astype(jnp.float32),
        precision=lax.Precision.HIGHEST,
        preferred_element_type=jnp.float32,
    )
    total = jnp.sum(jnp.where((lane >> 4) == row, wide, 0.0), axis=0, keepdims=True)
    out[...] = jnp.broadcast_to(total, out.shape)


def logits_kernel(start, stop, hidden, weight, *more):
    part = jnp.dot(
        hidden[:, start:stop], weight[start:stop], preferred_element_type=jnp.float32
    )
    if start == 0:
        more[0][...] = part
    else:
        more[1][...] = more[0][...] + part


def share_kernel(start, stop, length, hidden, weight, logits, share, slope):
    rows = hidden.shape[0]
    part = jnp.dot(
        hidden[:, start:stop], weight[start:stop], preferred_element_type=jnp.float32
    )
    scores = jax.nn.sigmoid(logits[...] + part)
    inverse = 1.0 / jnp.sum(scores, axis=1, keepdims=True)
    position = lax.axis_index(CTX) * rows + lax.broadcasted_iota(jnp.int32, (rows, 1), 0)
    value = jnp.where(position < length[0], scores * inverse, 0.0)
    share[...] = value
    slope[...] = value * (1.0 - scores)


def grad_logits_kernel(length, share, slope, counts, theirs, mine, balance, turned):
    core = lax.axis_index("core")
    live = length[0].astype(jnp.float32)
    fraction = E * counts[:1] / (TOPK * live)
    weights = loss_scale * fraction / live
    weighted = jnp.sum(weights * share[...], axis=1, keepdims=True)
    turned[...] = ((weights - weighted) * slope[...]).T
    balance[...] = jnp.broadcast_to(
        jnp.sum(weighted, axis=0, keepdims=True) / loss_scale, balance.shape
    )
    for out, half in ((theirs, 1 - core), (mine, core)):
        value = turned[ds(half * HALF, HALF), :]
        high = value.astype(jnp.bfloat16)
        out[:HALF, :] = high
        out[HALF:, :] = (value - high.astype(jnp.float32)).astype(jnp.bfloat16)


def places():
    y, x, core = lax.axis_index("y"), lax.axis_index("x"), lax.axis_index("core")
    return jnp.where(core == 0, y, x), jnp.where(core == 0, x, y)


GROUPS = {
    "S": ((2, 0), (2, 1), (2, 2), (2, 3)),
    "O": ((1, 0), (1, 1), (3, 2), (3, 3)),
    "M": ((3, 0), (3, 1), (1, 2), (1, 3)),
    "W": ((0, 0), (0, 1), (0, 2), (0, 3)),
}
LOW, HIGH = slice(0, 896), slice(896, 1792)


def product_kernel(group, own, grad, hidden, out, whole):
    over_y = lax.axis_index("core") == (0 if own else 1)
    place = jnp.where(over_y, lax.axis_index("y"), lax.axis_index("x"))
    for n, (k, q) in enumerate(GROUPS[group]):
        p = place ^ k
        start = jnp.where(over_y, p * 1792 + q * 448, q * 1792 + p * 448)
        skip = start & 64
        columns = hidden[:, pl.ds(pl.multiple_of(start - skip, HALF), 512)]
        both = jnp.dot(grad[...], columns, preferred_element_type=jnp.float32)
        whole[n] = (both[:HALF] + both[HALF:]).T
        out[n * 448 : n * 448 + 448, :] = whole[n, ds(skip, 448), :]


def lead_kernel(mine, theirs, balance, s1, s3):
    s1[:896] = mine[LOW] + theirs[LOW]
    s1[896:904] = balance[...]
    s3[...] = mine[HIGH] + theirs[HIGH]


def direct_kernel(mine, theirs, o1, o3):
    o1[...] = mine[LOW] + theirs[LOW]
    o3[...] = mine[HIGH] + theirs[HIGH]


def relay_kernel(mine, theirs, balance, r1, r3, m1, m3):
    m1[...] = mine[HIGH] + theirs[HIGH] + r3[...]
    m3[:896] = mine[LOW] + theirs[LOW] + r1[:896]
    m3[896:904] = balance[...] + r1[896:904]


def second_kernel(mine, theirs, o1, m3, m1, o3, balance, r1, *outs):
    _, q = places()
    sum_so_far = balance[...] + r1[896:904] + m3[896:904]
    for upper in range(2):

        @pl.when(q // 2 == upper)
        def _():
            for k, out in enumerate(outs):
                arrived = (o1, m3) if upper ^ (k >> 1) == 0 else (m1, o3)
                own = ds((q ^ k) * 448, 448)
                rows = ds(((q ^ k) & 1) * 448, 448)
                out[:448] = mine[own] + theirs[own] + arrived[0][rows] + arrived[1][rows]

    for out in outs:
        out[448:456] = sum_so_far


def join_kernel(a0, a1, a2, a3, same, other):
    zh = lax.axis_index("zh")
    for out, z in ((same, zh), (other, 1 - zh)):
        rows = ds(z * 224, 224)
        out[:224] = a0[rows] + a1[rows] + a2[rows] + a3[rows]
        out[224:232] = a0[448:456] + a1[448:456] + a2[448:456] + a3[448:456]


def half_kernel(same, r1, r2, r3, half):
    half[...] = same[:224] + r1[:224] + r2[:224] + r3[:224]


def balance_kernel(same, r2, balance):
    balance[0] = jnp.sum(same[224:225, :1] + r2[224:225, :1])


def last_kernel(half, peer, out):
    core = lax.axis_index("core")
    out[:, pl.ds(pl.multiple_of(core * HALF, HALF), HALF)] = half[...]
    out[:, pl.ds(pl.multiple_of((1 - core) * HALF, HALF), HALF)] = peer[...]


def shards(hidden, router_weight, expert_index, lengths):
    rows, width = hidden.shape

    counts = local(
        count_kernel,
        f32(8, E),
        lengths,
        expert_index.T,
        scalars=1,
        limit=4,
        cost_estimate=pl.CostEstimate(flops=10**10, bytes_accessed=10**7, transcendentals=0),
    )
    hidden = pltpu.with_memory_space_constraint(hidden, pltpu.VMEM)
    router_weight = pltpu.with_memory_space_constraint(router_weight, pltpu.VMEM)
    cuts = (0, 0, width // 2, width)
    parts = ()
    for n, (axis, steps) in enumerate((("y", (2, 1, 3)), ("x", (2, 1, 3)), (Z, (2,)))):
        arrived = [swap(counts, axis, k) for k in steps]
        low, high = cuts[n : n + 2]
        if high > low:
            final = high == width
            parts = local(
                functools.partial(share_kernel if final else logits_kernel, low, high),
                (f32(rows, E),) * (2 if final else 1),
                *((lengths,) if final else ()),
                hidden,
                router_weight,
                *parts,
                scalars=1 if final else 0,
                limit=4,
                cost_estimate=pl.CostEstimate(
                    flops=2 * rows * (high - low) * E,
                    bytes_accessed=2 * rows * (high - low),
                    transcendentals=0,
                ),
                input_output_aliases={2 + final: 0} if parts else {},
            )
        counts = functools.reduce(jnp.add, arrived, counts)
    share, slope = parts

    split = jax.ShapeDtypeStruct((E, rows), jnp.bfloat16)
    grad_theirs, grad_mine, balance = local(
        grad_logits_kernel,
        (split, split, f32(8, HALF)),
        lengths,
        share,
        slope,
        counts,
        scalars=1,
        limit=6,
        scratch_shapes=[pltpu.VMEM((E, rows), jnp.float32)],
    )

    def product(grad, group, own):
        work = pl.CostEstimate(flops=width * E, bytes_accessed=width, transcendentals=0)
        return local(
            functools.partial(product_kernel, group, own),
            f32(width // 4, HALF),
            grad,
            hidden,
            cost_estimate=work,
            limit=4,
            scratch_shapes=[pltpu.VMEM((4, 512, HALF), jnp.float32)],
        )

    mine, theirs = {}, {}

    def make_theirs(group):
        made = product(grad_theirs, group, False)
        theirs[group] = swap(made, "core", 1)

    def make_mine(group):
        mine[group] = product(grad_mine, group, True)

    make_theirs("S")
    make_theirs("O")
    make_mine("S")
    s1, s3 = local(lead_kernel, (f32(904, HALF), f32(896, HALF)), mine["S"], theirs["S"], balance)
    r1, r3 = cross(s1, 0, 1), cross(s3, 0, 3)
    make_theirs("M")
    make_mine("O")
    o1, o3 = local(direct_kernel, (f32(896, HALF), f32(896, HALF)), mine["O"], theirs["O"])
    o1, o3 = cross(o1, 0, 1), cross(o3, 0, 3)
    make_mine("M")
    m1, m3 = local(
        relay_kernel, (f32(896, HALF), f32(904, HALF)), mine["M"], theirs["M"], balance, r1, r3
    )
    m1 = cross(m1, 0, 1)
    m3 = cross(m3, 0, 3)
    make_theirs("W")
    make_mine("W")
    a = local(
        second_kernel, (f32(456, HALF),) * 4, mine["W"], theirs["W"], o1, m3, m1, o3, balance, r1
    )
    arrived = {}
    for k in (2, 1, 3):
        arrived[k] = cross(a[k], 1, k)
    same, other = local(
        join_kernel, (f32(232, HALF),) * 2, a[0], arrived[1], arrived[2], arrived[3]
    )
    for k in (2, 1, 3):
        arrived[k] = swap(other if k > 1 else same, Z, k)
    half = local(half_kernel, f32(224, HALF), same, arrived[1], arrived[2], arrived[3])
    peer = swap(half, "core", 1)
    balance = local(balance_kernel, f32(1), same, arrived[2], out_specs=SMEM)
    return local(last_kernel, f32(224, E), half, peer), balance


def solution(mesh):
    finer = Mesh(mesh.devices.reshape(2, 2, 4, 4, 2), MESH)
    rows = MESH

    return jax.shard_map(
        shards,
        mesh=finer,
        in_specs=(P(rows, None), P(), P(rows, None), P(("zl", "core"))),
        out_specs=(P(CTX, None), P(("zl", "core"))),
        check_vma=False,
    )
```

```python
import functools
import itertools

import jax
import jax.numpy as jnp
from jax import lax
from jax.experimental import pallas as pl
from jax.experimental.pallas import tpu as pltpu
from jax.sharding import Mesh
from jax.sharding import PartitionSpec as P

E = 256
TOPK = 8
HALF = 128
loss_scale = 65536.0

MESH = ("zl", "core", "y", "x", "zh")
CTX = ("y", "x", "zh")
Z = ("zl", "zh")


MIB = 1 << 20
VMEM = pl.BlockSpec(memory_space=pltpu.VMEM)
SMEM = pl.BlockSpec(memory_space=pltpu.SMEM)


def f32(*dims):
    return jax.ShapeDtypeStruct(dims, jnp.float32)


def local(kernel, outs, *args, scalars=0, limit=2, **more):
    specs = (VMEM,) * len(outs) if isinstance(outs, tuple) else VMEM
    return pl.pallas_call(
        kernel,
        out_shape=outs,
        in_specs=[SMEM] * scalars + [VMEM] * (len(args) - scalars),
        out_specs=more.pop("out_specs", specs),
        compiler_params=pltpu.CompilerParams(vmem_limit_bytes=limit * MIB),
        **more,
    )(*args)


def swap(array, axis, k):
    if axis == Z:
        pairs = [(l * 2 + h, (l ^ (k & 1)) * 2 + (h ^ (k >> 1))) for l in range(2) for h in range(2)]
    elif axis == "core":
        pairs = [(0, 1), (1, 0)]
    else:
        pairs = [(i, i ^ k) for i in range(4)]
    return lax.ppermute(array, axis, pairs)


SHAPE = (2, 2, 4, 4, 2)


def flat(place):
    return functools.reduce(lambda n, i: n * SHAPE[i] + place[i], range(5), 0)


def cross(array, stage, k):
    pairs = []
    for place in itertools.product(*map(range, SHAPE)):
        zl, core, y, x, zh = place
        role = core ^ ((y ^ x) & 1)
        if role == stage:
            y = y ^ k
        else:
            x = x ^ k
        pairs.append((flat(place), flat((zl, role ^ ((y ^ x) & 1), y, x, zh))))
    return lax.ppermute(array, MESH, pairs)


def role_here():
    y, x = lax.axis_index("y"), lax.axis_index("x")
    return lax.axis_index("core") ^ ((y ^ x) & 1)


def ds(start, size):
    return pl.ds(pl.multiple_of(start, 8), size)


def count_kernel(length, index, out):
    rows = index.shape[1]
    position = lax.axis_index(CTX) * rows + lax.broadcasted_iota(jnp.int32, (1, rows), 1)
    experts = jnp.where(position < length[0], index[...], -1)
    high, low = experts >> 4, experts & 15
    names = lax.broadcasted_iota(jnp.int32, (16, rows), 0)
    counts = jnp.zeros((16, 16), jnp.float32)
    for k in range(TOPK):
        one, two = (
            (part[k : k + 1, :] == names).astype(jnp.float32).astype(jnp.bfloat16)
            for part in (high, low)
        )
        counts = counts + lax.dot_general(
            one, two, (((1,), (1,)), ((), ())), preferred_element_type=jnp.float32
        )
    lane = lax.broadcasted_iota(jnp.int32, (16, E), 1)
    row = lax.broadcasted_iota(jnp.int32, (16, E), 0)
    wide = jnp.dot(
        counts,
        ((lane & 15) == row).astype(jnp.float32),
        precision=lax.Precision.HIGHEST,
        preferred_element_type=jnp.float32,
    )
    total = jnp.sum(jnp.where((lane >> 4) == row, wide, 0.0), axis=0, keepdims=True)
    out[...] = jnp.broadcast_to(total, out.shape)


def logits_kernel(start, stop, hidden, weight, *more):
    part = jnp.dot(
        hidden[:, start:stop], weight[start:stop], preferred_element_type=jnp.float32
    )
    if start == 0:
        more[0][...] = part
    else:
        more[1][...] = more[0][...] + part


def share_kernel(start, stop, length, hidden, weight, logits, share, slope):
    rows = hidden.shape[0]
    part = jnp.dot(
        hidden[:, start:stop], weight[start:stop], preferred_element_type=jnp.float32
    )
    scores = jax.nn.sigmoid(logits[...] + part)
    inverse = 1.0 / jnp.sum(scores, axis=1, keepdims=True)
    position = lax.axis_index(CTX) * rows + lax.broadcasted_iota(jnp.int32, (rows, 1), 0)
    value = jnp.where(position < length[0], scores * inverse, 0.0)
    share[...] = value
    slope[...] = value * (1.0 - scores)


def grad_logits_kernel(length, share, slope, counts, theirs, mine, balance, turned):
    live = length[0].astype(jnp.float32)
    fraction = E * counts[:1] / (TOPK * live)
    weights = loss_scale * fraction / live
    weighted = jnp.sum(weights * share[...], axis=1, keepdims=True)
    turned[...] = ((weights - weighted) * slope[...]).T
    mean = jnp.sum(weighted, axis=0, keepdims=True) / loss_scale
    owner = lax.broadcasted_iota(jnp.int32, balance.shape, 0) >> 2
    balance[...] = jnp.where(owner == lax.axis_index("core"), mean, 0.0)
    role = role_here()
    for out, half in ((theirs, 1 - role), (mine, role)):
        value = turned[ds(half * HALF, HALF), :]
        high = value.astype(jnp.bfloat16)
        out[:HALF, :] = high
        out[HALF:, :] = (value - high.astype(jnp.float32)).astype(jnp.bfloat16)


def places():
    y, x, role = lax.axis_index("y"), lax.axis_index("x"), role_here()
    return jnp.where(role == 0, y, x), jnp.where(role == 0, x, y)


GROUPS = {
    "S": ((2, 0), (2, 1), (2, 2), (2, 3)),
    "O": ((1, 0), (1, 1), (3, 2), (3, 3)),
    "M": ((3, 0), (3, 1), (1, 2), (1, 3)),
    "W": ((0, 0), (0, 1), (0, 2), (0, 3)),
}
LOW, HIGH = slice(0, 896), slice(896, 1792)


def product_kernel(group, own, grad, hidden, *more):
    *balance, out, whole = more
    if balance:
        out[1792:1800] = balance[0][...]
    over_y = role_here() == (0 if own else 1)
    place = jnp.where(over_y, lax.axis_index("y"), lax.axis_index("x"))
    for n, (k, q) in enumerate(GROUPS[group]):
        p = place ^ k
        start = jnp.where(over_y, p * 1792 + q * 448, q * 1792 + p * 448)
        skip = start & 64
        columns = hidden[:, pl.ds(pl.multiple_of(start - skip, HALF), 512)]
        both = jnp.dot(grad[...], columns, preferred_element_type=jnp.float32)
        whole[n] = (both[:HALF] + both[HALF:]).T
        out[n * 448 : n * 448 + 448, :] = whole[n, ds(skip, 448), :]


def lead_kernel(mine, theirs, balance, s1, s3, both):
    s1[:896] = mine[LOW] + theirs[LOW]
    s1[896:904] = balance[...] + theirs[1792:1800]
    both[...] = balance[...] + theirs[1792:1800]
    s3[...] = mine[HIGH] + theirs[HIGH]


def direct_kernel(mine, theirs, o1, o3):
    o1[...] = mine[LOW] + theirs[LOW]
    o3[...] = mine[HIGH] + theirs[HIGH]


def relay_kernel(mine, theirs, balance, r1, r3, m1, m3):
    m1[...] = mine[HIGH] + theirs[HIGH] + r3[...]
    m3[:896] = mine[LOW] + theirs[LOW] + r1[:896]
    m3[896:904] = balance[...] + r1[896:904]


def second_kernel(mine, theirs, o1, m3, m1, o3, balance, r1, *outs):
    _, q = places()
    sum_so_far = balance[...] + r1[896:904] + m3[896:904]
    for upper in range(2):

        @pl.when(q // 2 == upper)
        def _():
            for k, out in enumerate(outs):
                arrived = (o1, m3) if upper ^ (k >> 1) == 0 else (m1, o3)
                own = ds((q ^ k) * 448, 448)
                rows = ds(((q ^ k) & 1) * 448, 448)
                out[:448] = mine[own] + theirs[own] + arrived[0][rows] + arrived[1][rows]

    for out in outs:
        out[448:456] = sum_so_far


def join_kernel(a0, a1, a2, a3, same, other):
    zh = lax.axis_index("zh")
    for out, z in ((same, zh), (other, 1 - zh)):
        rows = ds(z * 224, 224)
        out[:224] = a0[rows] + a1[rows] + a2[rows] + a3[rows]
        out[224:232] = a0[448:456] + a1[448:456] + a2[448:456] + a3[448:456]


def half_kernel(same, r1, r2, r3, half):
    half[...] = same[:224] + r1[:224] + r2[:224] + r3[:224]


def balance_kernel(same, r2, balance):
    tile = same[224:232, :1] + r2[224:232, :1]
    balance[0] = jnp.sum(jnp.where(lax.axis_index("core") == 0, tile[:1], tile[4:5]))


def last_kernel(half, peer, out):
    role = role_here()
    out[:, pl.ds(pl.multiple_of(role * HALF, HALF), HALF)] = half[...]
    out[:, pl.ds(pl.multiple_of((1 - role) * HALF, HALF), HALF)] = peer[...]


def shards(hidden, router_weight, expert_index, lengths):
    rows, width = hidden.shape

    counts = local(
        count_kernel,
        f32(8, E),
        lengths,
        expert_index.T,
        scalars=1,
        limit=4,
        cost_estimate=pl.CostEstimate(flops=10**10, bytes_accessed=10**7, transcendentals=0),
    )
    hidden = pltpu.with_memory_space_constraint(hidden, pltpu.VMEM)
    router_weight = pltpu.with_memory_space_constraint(router_weight, pltpu.VMEM)
    cuts = (0, 0, width // 2, width)
    parts = ()
    for n, (axis, steps) in enumerate((("y", (2, 1, 3)), ("x", (2, 1, 3)), (Z, (2,)))):
        arrived = [swap(counts, axis, k) for k in steps]
        low, high = cuts[n : n + 2]
        if high > low:
            final = high == width
            parts = local(
                functools.partial(share_kernel if final else logits_kernel, low, high),
                (f32(rows, E),) * (2 if final else 1),
                *((lengths,) if final else ()),
                hidden,
                router_weight,
                *parts,
                scalars=1 if final else 0,
                limit=4,
                cost_estimate=pl.CostEstimate(
                    flops=2 * rows * (high - low) * E,
                    bytes_accessed=2 * rows * (high - low),
                    transcendentals=0,
                ),
                input_output_aliases={2 + final: 0} if parts else {},
            )
        counts = functools.reduce(jnp.add, arrived, counts)
    share, slope = parts

    split = jax.ShapeDtypeStruct((E, rows), jnp.bfloat16)
    grad_theirs, grad_mine, balance = local(
        grad_logits_kernel,
        (split, split, f32(8, HALF)),
        lengths,
        share,
        slope,
        counts,
        scalars=1,
        limit=6,
        scratch_shapes=[pltpu.VMEM((E, rows), jnp.float32)],
    )

    def product(grad, group, own, *more):
        work = pl.CostEstimate(flops=width * E, bytes_accessed=width, transcendentals=0)
        return local(
            functools.partial(product_kernel, group, own),
            f32(width // 4 + 8 * len(more), HALF),
            grad,
            hidden,
            *more,
            cost_estimate=work,
            limit=4,
            scratch_shapes=[pltpu.VMEM((4, 512, HALF), jnp.float32)],
        )

    mine, theirs = {}, {}

    def make_theirs(group):
        more = (balance,) if group == "S" else ()
        made = product(grad_theirs, group, False, *more)
        theirs[group] = swap(made, "core", 1)

    def make_mine(group):
        mine[group] = product(grad_mine, group, True)

    make_theirs("S")
    make_theirs("O")
    make_mine("S")
    s1, s3, balances = local(
        lead_kernel, (f32(904, HALF), f32(896, HALF), f32(8, HALF)), mine["S"], theirs["S"], balance
    )
    r1, r3 = cross(s1, 0, 1), cross(s3, 0, 3)
    make_theirs("M")
    make_mine("O")
    o1, o3 = local(direct_kernel, (f32(896, HALF), f32(896, HALF)), mine["O"], theirs["O"])
    o1, o3 = cross(o1, 0, 1), cross(o3, 0, 3)
    make_mine("M")
    m1, m3 = local(
        relay_kernel, (f32(896, HALF), f32(904, HALF)), mine["M"], theirs["M"], balances, r1, r3
    )
    m1 = cross(m1, 0, 1)
    m3 = cross(m3, 0, 3)
    make_theirs("W")
    make_mine("W")
    a = local(
        second_kernel, (f32(456, HALF),) * 4, mine["W"], theirs["W"], o1, m3, m1, o3, balances, r1
    )
    arrived = {}
    for k in (2, 1, 3):
        arrived[k] = cross(a[k], 1, k)
    same, other = local(
        join_kernel, (f32(232, HALF),) * 2, a[0], arrived[1], arrived[2], arrived[3]
    )
    for k in (2, 1, 3):
        arrived[k] = swap(other if k > 1 else same, Z, k)
    half = local(half_kernel, f32(224, HALF), same, arrived[1], arrived[2], arrived[3])
    peer = swap(half, "core", 1)
    balance = local(balance_kernel, f32(1), same, arrived[2], out_specs=SMEM)
    return local(last_kernel, f32(224, E), half, peer), balance


def solution(mesh):
    finer = Mesh(mesh.devices.reshape(2, 2, 4, 4, 2), MESH)
    rows = MESH

    return jax.shard_map(
        shards,
        mesh=finer,
        in_specs=(P(rows, None), P(), P(rows, None), P(("zl", "core"))),
        out_specs=(P(CTX, None), P(("zl", "core"))),
        check_vma=False,
    )
```

```python
import functools
import itertools

import jax
import jax.numpy as jnp
from jax import lax
from jax.experimental import pallas as pl
from jax.experimental.pallas import tpu as pltpu
from jax.sharding import Mesh
from jax.sharding import PartitionSpec as P

E = 256
TOPK = 8
HALF = 128
loss_scale = 65536.0

MESH = ("zl", "core", "y", "x", "zh")
CTX = ("y", "x", "zh")
Z = ("zl", "zh")


MIB = 1 << 20
VMEM = pl.BlockSpec(memory_space=pltpu.VMEM)
SMEM = pl.BlockSpec(memory_space=pltpu.SMEM)


def f32(*dims):
    return jax.ShapeDtypeStruct(dims, jnp.float32)


def local(kernel, outs, *args, scalars=0, limit=2, **more):
    specs = (VMEM,) * len(outs) if isinstance(outs, tuple) else VMEM
    return pl.pallas_call(
        kernel,
        out_shape=outs,
        in_specs=[SMEM] * scalars + [VMEM] * (len(args) - scalars),
        out_specs=more.pop("out_specs", specs),
        compiler_params=pltpu.CompilerParams(vmem_limit_bytes=limit * MIB),
        **more,
    )(*args)


def swap(array, axis, k):
    if axis == Z:
        pairs = [(l * 2 + h, (l ^ (k & 1)) * 2 + (h ^ (k >> 1))) for l in range(2) for h in range(2)]
    elif axis == "core":
        pairs = [(0, 1), (1, 0)]
    else:
        pairs = [(i, i ^ k) for i in range(4)]
    return lax.ppermute(array, axis, pairs)


SHAPE = (2, 2, 4, 4, 2)


def flat(place):
    return functools.reduce(lambda n, i: n * SHAPE[i] + place[i], range(5), 0)


def cross(array, stage, k):
    pairs = []
    for place in itertools.product(*map(range, SHAPE)):
        zl, core, y, x, zh = place
        role = core ^ ((y ^ x) & 1)
        if role == stage:
            y = y ^ k
        else:
            x = x ^ k
        pairs.append((flat(place), flat((zl, role ^ ((y ^ x) & 1), y, x, zh))))
    return lax.ppermute(array, MESH, pairs)


def turn(array, axis, k):
    at = MESH.index(axis)
    pairs = []
    for place in itertools.product(*map(range, SHAPE)):
        other = list(place)
        other[at] ^= k
        other[1] ^= k & 1
        pairs.append((flat(place), flat(other)))
    return lax.ppermute(array, MESH, pairs)


def role_here():
    y, x = lax.axis_index("y"), lax.axis_index("x")
    return lax.axis_index("core") ^ ((y ^ x) & 1)


def ds(start, size):
    return pl.ds(pl.multiple_of(start, 8), size)


def count_kernel(length, index, out):
    rows = index.shape[1]
    position = lax.axis_index(CTX) * rows + lax.broadcasted_iota(jnp.int32, (1, rows), 1)
    experts = jnp.where(position < length[0], index[...], -1)
    high, low = experts >> 4, experts & 15
    names = lax.broadcasted_iota(jnp.int32, (16, rows), 0)
    counts = jnp.zeros((16, 16), jnp.float32)
    for k in range(TOPK):
        one, two = (
            (part[k : k + 1, :] == names).astype(jnp.float32).astype(jnp.bfloat16)
            for part in (high, low)
        )
        counts = counts + lax.dot_general(
            one, two, (((1,), (1,)), ((), ())), preferred_element_type=jnp.float32
        )
    lane = lax.broadcasted_iota(jnp.int32, (16, E), 1)
    row = lax.broadcasted_iota(jnp.int32, (16, E), 0)
    wide = jnp.dot(
        counts,
        ((lane & 15) == row).astype(jnp.float32),
        precision=lax.Precision.HIGHEST,
        preferred_element_type=jnp.float32,
    )
    total = jnp.sum(jnp.where((lane >> 4) == row, wide, 0.0), axis=0, keepdims=True)
    out[...] = jnp.broadcast_to(total, out.shape)


def mix_kernel(counts, mixed, out):
    owner = lax.broadcasted_iota(jnp.int32, out.shape, 0) >> 2
    out[...] = jnp.where(owner == lax.axis_index("core"), counts[...], mixed[...])


def logits_kernel(start, stop, hidden, weight, *more):
    part = jnp.dot(
        hidden[:, start:stop], weight[start:stop], preferred_element_type=jnp.float32
    )
    if start == 0:
        more[0][...] = part
    else:
        more[1][...] = more[0][...] + part


def share_kernel(start, stop, length, hidden, weight, logits, share, slope):
    rows = hidden.shape[0]
    part = jnp.dot(
        hidden[:, start:stop], weight[start:stop], preferred_element_type=jnp.float32
    )
    scores = jax.nn.sigmoid(logits[...] + part)
    inverse = 1.0 / jnp.sum(scores, axis=1, keepdims=True)
    position = lax.axis_index(CTX) * rows + lax.broadcasted_iota(jnp.int32, (rows, 1), 0)
    value = jnp.where(position < length[0], scores * inverse, 0.0)
    share[...] = value
    slope[...] = value * (1.0 - scores)


def grad_logits_kernel(length, share, slope, counts, theirs, mine, balance, turned):
    live = length[0].astype(jnp.float32)
    mine_first = lax.axis_index("core") == 0
    fraction = E * jnp.where(mine_first, counts[:1], counts[4:5]) / (TOPK * live)
    weights = loss_scale * fraction / live
    weighted = jnp.sum(weights * share[...], axis=1, keepdims=True)
    turned[...] = ((weights - weighted) * slope[...]).T
    mean = jnp.sum(weighted, axis=0, keepdims=True) / loss_scale
    owner = lax.broadcasted_iota(jnp.int32, balance.shape, 0) >> 2
    balance[...] = jnp.where(owner == lax.axis_index("core"), mean, 0.0)
    role = role_here()
    for out, half in ((theirs, 1 - role), (mine, role)):
        value = turned[ds(half * HALF, HALF), :]
        high = value.astype(jnp.bfloat16)
        out[:HALF, :] = high
        out[HALF:, :] = (value - high.astype(jnp.float32)).astype(jnp.bfloat16)


def places():
    y, x, role = lax.axis_index("y"), lax.axis_index("x"), role_here()
    return jnp.where(role == 0, y, x), jnp.where(role == 0, x, y)


GROUPS = {
    "S": ((2, 0), (2, 1), (2, 2), (2, 3)),
    "O": ((1, 0), (1, 1), (3, 2), (3, 3)),
    "M": ((3, 0), (3, 1), (1, 2), (1, 3)),
    "W": ((0, 0), (0, 1), (0, 2), (0, 3)),
}
LOW, HIGH = slice(0, 896), slice(896, 1792)


def product_kernel(group, own, grad, hidden, *more):
    *balance, out, whole = more
    if balance:
        out[1792:1800] = balance[0][...]
    over_y = role_here() == (0 if own else 1)
    place = jnp.where(over_y, lax.axis_index("y"), lax.axis_index("x"))
    for n, (k, q) in enumerate(GROUPS[group]):
        p = place ^ k
        start = jnp.where(over_y, p * 1792 + q * 448, q * 1792 + p * 448)
        skip = start & 64
        columns = hidden[:, pl.ds(pl.multiple_of(start - skip, HALF), 512)]
        both = jnp.dot(grad[...], columns, preferred_element_type=jnp.float32)
        whole[n] = (both[:HALF] + both[HALF:]).T
        out[n * 448 : n * 448 + 448, :] = whole[n, ds(skip, 448), :]


def lead_kernel(mine, theirs, balance, s1, s3, both):
    s1[:896] = mine[LOW] + theirs[LOW]
    s1[896:904] = balance[...] + theirs[1792:1800]
    both[...] = balance[...] + theirs[1792:1800]
    s3[...] = mine[HIGH] + theirs[HIGH]


def direct_kernel(mine, theirs, o1, o3):
    o1[...] = mine[LOW] + theirs[LOW]
    o3[...] = mine[HIGH] + theirs[HIGH]


def relay_kernel(mine, theirs, balance, r1, r3, m1, m3):
    m1[...] = mine[HIGH] + theirs[HIGH] + r3[...]
    m3[:896] = mine[LOW] + theirs[LOW] + r1[:896]
    m3[896:904] = balance[...] + r1[896:904]


def second_kernel(mine, theirs, o1, m3, m1, o3, balance, r1, *outs):
    _, q = places()
    sum_so_far = balance[...] + r1[896:904] + m3[896:904]
    for upper in range(2):

        @pl.when(q // 2 == upper)
        def _():
            for k, out in enumerate(outs):
                arrived = (o1, m3) if upper ^ (k >> 1) == 0 else (m1, o3)
                own = ds((q ^ k) * 448, 448)
                rows = ds(((q ^ k) & 1) * 448, 448)
                out[:448] = mine[own] + theirs[own] + arrived[0][rows] + arrived[1][rows]

    for out in outs:
        out[448:456] = sum_so_far


def join_kernel(a0, a1, a2, a3, same, other):
    zh = lax.axis_index("zh")
    for out, z in ((same, zh), (other, 1 - zh)):
        rows = ds(z * 224, 224)
        out[:224] = a0[rows] + a1[rows] + a2[rows] + a3[rows]
        out[224:232] = a0[448:456] + a1[448:456] + a2[448:456] + a3[448:456]


def half_kernel(same, r1, r2, r3, half):
    half[...] = same[:224] + r1[:224] + r2[:224] + r3[:224]


def balance_kernel(same, r2, balance):
    tile = same[224:232, :1] + r2[224:232, :1]
    balance[0] = jnp.sum(jnp.where(lax.axis_index("core") == 0, tile[:1], tile[4:5]))


def last_kernel(half, peer, out):
    role = role_here()
    out[:, pl.ds(pl.multiple_of(role * HALF, HALF), HALF)] = half[...]
    out[:, pl.ds(pl.multiple_of((1 - role) * HALF, HALF), HALF)] = peer[...]


def shards(hidden, router_weight, expert_index, lengths):
    rows, width = hidden.shape

    counts = local(
        count_kernel,
        f32(8, E),
        lengths,
        expert_index.T,
        scalars=1,
        limit=4,
        cost_estimate=pl.CostEstimate(flops=10**10, bytes_accessed=10**7, transcendentals=0),
    )
    hidden = pltpu.with_memory_space_constraint(hidden, pltpu.VMEM)
    router_weight = pltpu.with_memory_space_constraint(router_weight, pltpu.VMEM)
    mixed = swap(counts, "core", 1)
    counts = local(mix_kernel, f32(8, E), counts, mixed)
    cuts = (0, 0, width // 2, width)
    parts = ()
    for n, (axis, steps) in enumerate((("y", (2, 1, 3)), ("x", (2, 1, 3)), (Z, (2,)))):
        go = swap if axis == Z else turn
        arrived = [go(counts, axis, k) for k in steps]
        low, high = cuts[n : n + 2]
        if high > low:
            final = high == width
            parts = local(
                functools.partial(share_kernel if final else logits_kernel, low, high),
                (f32(rows, E),) * (2 if final else 1),
                *((lengths,) if final else ()),
                hidden,
                router_weight,
                *parts,
                scalars=1 if final else 0,
                limit=4,
                cost_estimate=pl.CostEstimate(
                    flops=2 * rows * (high - low) * E,
                    bytes_accessed=2 * rows * (high - low),
                    transcendentals=0,
                ),
                input_output_aliases={2 + final: 0} if parts else {},
            )
        counts = functools.reduce(jnp.add, arrived, counts)
    share, slope = parts

    split = jax.ShapeDtypeStruct((E, rows), jnp.bfloat16)
    grad_theirs, grad_mine, balance = local(
        grad_logits_kernel,
        (split, split, f32(8, HALF)),
        lengths,
        share,
        slope,
        counts,
        scalars=1,
        limit=6,
        scratch_shapes=[pltpu.VMEM((E, rows), jnp.float32)],
    )

    def product(grad, group, own, *more):
        work = pl.CostEstimate(flops=width * E, bytes_accessed=width, transcendentals=0)
        return local(
            functools.partial(product_kernel, group, own),
            f32(width // 4 + 8 * len(more), HALF),
            grad,
            hidden,
            *more,
            cost_estimate=work,
            limit=4,
            scratch_shapes=[pltpu.VMEM((4, 512, HALF), jnp.float32)],
        )

    mine, theirs = {}, {}

    def make_theirs(group):
        more = (balance,) if group == "S" else ()
        made = product(grad_theirs, group, False, *more)
        theirs[group] = swap(made, "core", 1)

    def make_mine(group):
        mine[group] = product(grad_mine, group, True)

    make_theirs("S")
    make_theirs("O")
    make_mine("S")
    s1, s3, balances = local(
        lead_kernel, (f32(904, HALF), f32(896, HALF), f32(8, HALF)), mine["S"], theirs["S"], balance
    )
    r1, r3 = cross(s1, 0, 1), cross(s3, 0, 3)
    make_theirs("M")
    make_mine("O")
    o1, o3 = local(direct_kernel, (f32(896, HALF), f32(896, HALF)), mine["O"], theirs["O"])
    o1, o3 = cross(o1, 0, 1), cross(o3, 0, 3)
    make_mine("M")
    m1, m3 = local(
        relay_kernel, (f32(896, HALF), f32(904, HALF)), mine["M"], theirs["M"], balances, r1, r3
    )
    m1 = cross(m1, 0, 1)
    m3 = cross(m3, 0, 3)
    make_theirs("W")
    make_mine("W")
    a = local(
        second_kernel, (f32(456, HALF),) * 4, mine["W"], theirs["W"], o1, m3, m1, o3, balances, r1
    )
    arrived = {}
    for k in (2, 1, 3):
        arrived[k] = cross(a[k], 1, k)
    same, other = local(
        join_kernel, (f32(232, HALF),) * 2, a[0], arrived[1], arrived[2], arrived[3]
    )
    for k in (2, 1, 3):
        arrived[k] = swap(other if k > 1 else same, Z, k)
    half = local(half_kernel, f32(224, HALF), same, arrived[1], arrived[2], arrived[3])
    peer = swap(half, "core", 1)
    balance = local(balance_kernel, f32(1), same, arrived[2], out_specs=SMEM)
    return local(last_kernel, f32(224, E), half, peer), balance


def solution(mesh):
    finer = Mesh(mesh.devices.reshape(2, 2, 4, 4, 2), MESH)
    rows = MESH

    return jax.shard_map(
        shards,
        mesh=finer,
        in_specs=(P(rows, None), P(), P(rows, None), P(("zl", "core"))),
        out_specs=(P(CTX, None), P(("zl", "core"))),
        check_vma=False,
    )
```

```python
import functools
import itertools

import jax
import jax.numpy as jnp
from jax import lax
from jax.experimental import pallas as pl
from jax.experimental.pallas import tpu as pltpu
from jax.sharding import Mesh
from jax.sharding import PartitionSpec as P

E = 256
TOPK = 8
HALF = 128
loss_scale = 65536.0

MESH = ("zl", "core", "y", "x", "zh")
CTX = ("y", "x", "zh")
Z = ("zl", "zh")


MIB = 1 << 20
VMEM = pl.BlockSpec(memory_space=pltpu.VMEM)
SMEM = pl.BlockSpec(memory_space=pltpu.SMEM)


def f32(*dims):
    return jax.ShapeDtypeStruct(dims, jnp.float32)


def local(kernel, outs, *args, scalars=0, limit=2, **more):
    specs = (VMEM,) * len(outs) if isinstance(outs, tuple) else VMEM
    return pl.pallas_call(
        kernel,
        out_shape=outs,
        in_specs=[SMEM] * scalars + [VMEM] * (len(args) - scalars),
        out_specs=more.pop("out_specs", specs),
        compiler_params=pltpu.CompilerParams(vmem_limit_bytes=limit * MIB),
        **more,
    )(*args)


def swap(array, axis, k):
    if axis == Z:
        pairs = [(l * 2 + h, (l ^ (k & 1)) * 2 + (h ^ (k >> 1))) for l in range(2) for h in range(2)]
    elif axis == "core":
        pairs = [(0, 1), (1, 0)]
    else:
        pairs = [(i, i ^ k) for i in range(4)]
    return lax.ppermute(array, axis, pairs)


SHAPE = (2, 2, 4, 4, 2)


def flat(place):
    return functools.reduce(lambda n, i: n * SHAPE[i] + place[i], range(5), 0)


def cross(array, stage, k):
    pairs = []
    for place in itertools.product(*map(range, SHAPE)):
        zl, core, y, x, zh = place
        role = core ^ ((y ^ x ^ zl) & 1)
        if role == stage:
            y = y ^ k
        else:
            x = x ^ k
        pairs.append((flat(place), flat((zl, role ^ ((y ^ x ^ zl) & 1), y, x, zh))))
    return lax.ppermute(array, MESH, pairs)


def turn(array, axis, k):
    at = MESH.index(axis)
    pairs = []
    for place in itertools.product(*map(range, SHAPE)):
        other = list(place)
        other[at] ^= k
        other[1] ^= k & 1
        pairs.append((flat(place), flat(other)))
    return lax.ppermute(array, MESH, pairs)


def over_z(array, k):
    pairs = []
    for place in itertools.product(*map(range, SHAPE)):
        zl, core, y, x, zh = place
        pairs.append((flat(place), flat((zl ^ (k & 1), core ^ (k & 1), y, x, zh ^ (k >> 1)))))
    return lax.ppermute(array, MESH, pairs)


def role_here():
    y, x, zl = lax.axis_index("y"), lax.axis_index("x"), lax.axis_index("zl")
    return lax.axis_index("core") ^ ((y ^ x ^ zl) & 1)


def ds(start, size):
    return pl.ds(pl.multiple_of(start, 8), size)


def count_kernel(length, index, out):
    rows = index.shape[1]
    position = lax.axis_index(CTX) * rows + lax.broadcasted_iota(jnp.int32, (1, rows), 1)
    experts = jnp.where(position < length[0], index[...], -1)
    high, low = experts >> 4, experts & 15
    names = lax.broadcasted_iota(jnp.int32, (16, rows), 0)
    counts = jnp.zeros((16, 16), jnp.float32)
    for k in range(TOPK):
        one, two = (
            (part[k : k + 1, :] == names).astype(jnp.float32).astype(jnp.bfloat16)
            for part in (high, low)
        )
        counts = counts + lax.dot_general(
            one, two, (((1,), (1,)), ((), ())), preferred_element_type=jnp.float32
        )
    lane = lax.broadcasted_iota(jnp.int32, (16, E), 1)
    row = lax.broadcasted_iota(jnp.int32, (16, E), 0)
    wide = jnp.dot(
        counts,
        ((lane & 15) == row).astype(jnp.float32),
        precision=lax.Precision.HIGHEST,
        preferred_element_type=jnp.float32,
    )
    total = jnp.sum(jnp.where((lane >> 4) == row, wide, 0.0), axis=0, keepdims=True)
    out[...] = jnp.broadcast_to(total, out.shape)


def mix_kernel(counts, mixed, out):
    owner = lax.broadcasted_iota(jnp.int32, out.shape, 0) >> 2
    out[...] = jnp.where(owner == lax.axis_index("core"), counts[...], mixed[...])


def logits_kernel(start, stop, hidden, weight, *more):
    part = jnp.dot(
        hidden[:, start:stop], weight[start:stop], preferred_element_type=jnp.float32
    )
    if start == 0:
        more[0][...] = part
    else:
        more[1][...] = more[0][...] + part


def share_kernel(start, stop, length, hidden, weight, logits, share, slope):
    rows = hidden.shape[0]
    part = jnp.dot(
        hidden[:, start:stop], weight[start:stop], preferred_element_type=jnp.float32
    )
    scores = jax.nn.sigmoid(logits[...] + part)
    inverse = 1.0 / jnp.sum(scores, axis=1, keepdims=True)
    position = lax.axis_index(CTX) * rows + lax.broadcasted_iota(jnp.int32, (rows, 1), 0)
    value = jnp.where(position < length[0], scores * inverse, 0.0)
    share[...] = value
    slope[...] = value * (1.0 - scores)


def grad_logits_kernel(length, share, slope, counts, theirs, mine, balance, turned):
    live = length[0].astype(jnp.float32)
    mine_first = lax.axis_index("core") == 0
    fraction = E * jnp.where(mine_first, counts[:1], counts[4:5]) / (TOPK * live)
    weights = loss_scale * fraction / live
    weighted = jnp.sum(weights * share[...], axis=1, keepdims=True)
    turned[...] = ((weights - weighted) * slope[...]).T
    mean = jnp.sum(weighted, axis=0, keepdims=True) / loss_scale
    owner = lax.broadcasted_iota(jnp.int32, balance.shape, 0) >> 2
    balance[...] = jnp.where(owner == lax.axis_index("core"), mean, 0.0)
    role = role_here()
    for out, half in ((theirs, 1 - role), (mine, role)):
        value = turned[ds(half * HALF, HALF), :]
        high = value.astype(jnp.bfloat16)
        out[:HALF, :] = high
        out[HALF:, :] = (value - high.astype(jnp.float32)).astype(jnp.bfloat16)


def places():
    y, x, role = lax.axis_index("y"), lax.axis_index("x"), role_here()
    return jnp.where(role == 0, y, x), jnp.where(role == 0, x, y)


GROUPS = {
    "S": ((2, 0), (2, 1), (2, 2), (2, 3)),
    "O": ((1, 0), (1, 1), (3, 2), (3, 3)),
    "M": ((3, 0), (3, 1), (1, 2), (1, 3)),
    "W": ((0, 0), (0, 1), (0, 2), (0, 3)),
}
LOW, HIGH = slice(0, 896), slice(896, 1792)


def product_kernel(group, own, grad, hidden, *more):
    *balance, out, whole = more
    if balance:
        out[1792:1800] = balance[0][...]
    over_y = role_here() == (0 if own else 1)
    place = jnp.where(over_y, lax.axis_index("y"), lax.axis_index("x"))
    for n, (k, q) in enumerate(GROUPS[group]):
        p = place ^ k
        start = jnp.where(over_y, p * 1792 + q * 448, q * 1792 + p * 448)
        skip = start & 64
        columns = hidden[:, pl.ds(pl.multiple_of(start - skip, HALF), 512)]
        both = jnp.dot(grad[...], columns, preferred_element_type=jnp.float32)
        whole[n] = (both[:HALF] + both[HALF:]).T
        out[n * 448 : n * 448 + 448, :] = whole[n, ds(skip, 448), :]


def lead_kernel(mine, theirs, balance, s1, s3, both):
    s1[:896] = mine[LOW] + theirs[LOW]
    s1[896:904] = balance[...] + theirs[1792:1800]
    both[...] = balance[...] + theirs[1792:1800]
    s3[...] = mine[HIGH] + theirs[HIGH]


def direct_kernel(mine, theirs, o1, o3):
    o1[...] = mine[LOW] + theirs[LOW]
    o3[...] = mine[HIGH] + theirs[HIGH]


def relay_kernel(mine, theirs, balance, r1, r3, m1, m3):
    m1[...] = mine[HIGH] + theirs[HIGH] + r3[...]
    m3[:896] = mine[LOW] + theirs[LOW] + r1[:896]
    m3[896:904] = balance[...] + r1[896:904]


def second_kernel(mine, theirs, o1, m3, m1, o3, balance, r1, *outs):
    _, q = places()
    sum_so_far = balance[...] + r1[896:904] + m3[896:904]
    for upper in range(2):

        @pl.when(q // 2 == upper)
        def _():
            for k, out in enumerate(outs):
                arrived = (o1, m3) if upper ^ (k >> 1) == 0 else (m1, o3)
                own = ds((q ^ k) * 448, 448)
                rows = ds(((q ^ k) & 1) * 448, 448)
                out[:448] = mine[own] + theirs[own] + arrived[0][rows] + arrived[1][rows]

    for out in outs:
        out[448:456] = sum_so_far


def join_kernel(a0, a1, a2, a3, same, other):
    zh = lax.axis_index("zh")
    for out, z in ((same, zh), (other, 1 - zh)):
        rows = ds(z * 224, 224)
        out[:224] = a0[rows] + a1[rows] + a2[rows] + a3[rows]
        out[224:232] = a0[448:456] + a1[448:456] + a2[448:456] + a3[448:456]


def half_kernel(same, r1, r2, r3, half):
    half[...] = same[:224] + r1[:224] + r2[:224] + r3[:224]


def balance_kernel(same, r2, balance):
    tile = same[224:232, :1] + r2[224:232, :1]
    balance[0] = jnp.sum(jnp.where(lax.axis_index("core") == 0, tile[:1], tile[4:5]))


def last_kernel(half, peer, out):
    role = role_here()
    out[:, pl.ds(pl.multiple_of(role * HALF, HALF), HALF)] = half[...]
    out[:, pl.ds(pl.multiple_of((1 - role) * HALF, HALF), HALF)] = peer[...]


def shards(hidden, router_weight, expert_index, lengths):
    rows, width = hidden.shape

    counts = local(
        count_kernel,
        f32(8, E),
        lengths,
        expert_index.T,
        scalars=1,
        limit=4,
        cost_estimate=pl.CostEstimate(flops=10**10, bytes_accessed=10**7, transcendentals=0),
    )
    hidden = pltpu.with_memory_space_constraint(hidden, pltpu.VMEM)
    router_weight = pltpu.with_memory_space_constraint(router_weight, pltpu.VMEM)
    mixed = swap(counts, "core", 1)
    counts = local(mix_kernel, f32(8, E), counts, mixed)
    cuts = (0, 0, width // 2, width)
    parts = ()
    for n, (axis, steps) in enumerate((("y", (2, 1, 3)), ("x", (2, 1, 3)), (Z, (2,)))):
        go = swap if axis == Z else turn
        arrived = [go(counts, axis, k) for k in steps]
        low, high = cuts[n : n + 2]
        if high > low:
            final = high == width
            parts = local(
                functools.partial(share_kernel if final else logits_kernel, low, high),
                (f32(rows, E),) * (2 if final else 1),
                *((lengths,) if final else ()),
                hidden,
                router_weight,
                *parts,
                scalars=1 if final else 0,
                limit=4,
                cost_estimate=pl.CostEstimate(
                    flops=2 * rows * (high - low) * E,
                    bytes_accessed=2 * rows * (high - low),
                    transcendentals=0,
                ),
                input_output_aliases={2 + final: 0} if parts else {},
            )
        counts = functools.reduce(jnp.add, arrived, counts)
    share, slope = parts

    split = jax.ShapeDtypeStruct((E, rows), jnp.bfloat16)
    grad_theirs, grad_mine, balance = local(
        grad_logits_kernel,
        (split, split, f32(8, HALF)),
        lengths,
        share,
        slope,
        counts,
        scalars=1,
        limit=6,
        scratch_shapes=[pltpu.VMEM((E, rows), jnp.float32)],
    )

    def product(grad, group, own, *more):
        work = pl.CostEstimate(flops=width * E, bytes_accessed=width, transcendentals=0)
        return local(
            functools.partial(product_kernel, group, own),
            f32(width // 4 + 8 * len(more), HALF),
            grad,
            hidden,
            *more,
            cost_estimate=work,
            limit=4,
            scratch_shapes=[pltpu.VMEM((4, 512, HALF), jnp.float32)],
        )

    mine, theirs = {}, {}

    def make_theirs(group):
        more = (balance,) if group == "S" else ()
        made = product(grad_theirs, group, False, *more)
        theirs[group] = swap(made, "core", 1)

    def make_mine(group):
        mine[group] = product(grad_mine, group, True)

    make_theirs("S")
    make_theirs("O")
    make_mine("S")
    s1, s3, balances = local(
        lead_kernel, (f32(904, HALF), f32(896, HALF), f32(8, HALF)), mine["S"], theirs["S"], balance
    )
    r1, r3 = cross(s1, 0, 1), cross(s3, 0, 3)
    make_theirs("M")
    make_mine("O")
    o1, o3 = local(direct_kernel, (f32(896, HALF), f32(896, HALF)), mine["O"], theirs["O"])
    o1, o3 = cross(o1, 0, 1), cross(o3, 0, 3)
    make_mine("M")
    m1, m3 = local(
        relay_kernel, (f32(896, HALF), f32(904, HALF)), mine["M"], theirs["M"], balances, r1, r3
    )
    m1 = cross(m1, 0, 1)
    m3 = cross(m3, 0, 3)
    make_theirs("W")
    make_mine("W")
    a = local(
        second_kernel, (f32(456, HALF),) * 4, mine["W"], theirs["W"], o1, m3, m1, o3, balances, r1
    )
    arrived = {}
    for k in (2, 1, 3):
        arrived[k] = cross(a[k], 1, k)
    same, other = local(
        join_kernel, (f32(232, HALF),) * 2, a[0], arrived[1], arrived[2], arrived[3]
    )
    for k in (2, 1, 3):
        arrived[k] = over_z(other if k > 1 else same, k)
    half = local(half_kernel, f32(224, HALF), same, arrived[1], arrived[2], arrived[3])
    peer = swap(half, "core", 1)
    balance = local(balance_kernel, f32(1), same, arrived[2], out_specs=SMEM)
    return local(last_kernel, f32(224, E), half, peer), balance


def solution(mesh):
    finer = Mesh(mesh.devices.reshape(2, 2, 4, 4, 2), MESH)
    rows = MESH

    return jax.shard_map(
        shards,
        mesh=finer,
        in_specs=(P(rows, None), P(), P(rows, None), P(("zl", "core"))),
        out_specs=(P(CTX, None), P(("zl", "core"))),
        check_vma=False,
    )
```
